32 devices in a mesh: dop: 8 (over z, y), slow: 4 (over x, core).
Axes of the slice: x: 2, y: 2, z: 4, core: 2. Of those that a mesh axis runs over, the one named last changes fastest.
Arguments:
- profiles: bfloat16 [32, 2, 1024, 2048], P('slow', None, 'dop'), may hold values from -6 to 6
- range_walk: int32 [2048], replicated, may hold values from -32 to 32
- band_order: int32 [32], replicated, may hold values from 0 to 31, each once
Outputs:
- ambiguity: float32 [2048, 1024], P(('dop', 'slow'))
The draws below stay inside these ranges and needn't reach their ends.
Inputs may be any that keep to these rules, and one draw needn't show every extreme that they name: `band_order`: each band number appears exactly once.
All inputs are finite; a program needn't handle non-finite values.
Results may differ from the reference program's by a relative error of at most 0.00067.
Values sent between devices are 32-bit elements; how exact they have to be, the bound alone decides.
A program may use at most 128 MiB of HBM per device.

```python
import math
import jax
import jax.numpy as jnp
from jax import lax

F = 2048
R = 1024
WALK = 32
BATCHES = 32
BANDS = 32
BAND_ROWS = 64


def plant(result, own_key, smallest, top_value):
    dims = result.shape
    index_at = [jax.random.randint(jax.random.fold_in(own_key, axis), (), 0, dims[axis]) for axis in range(len(dims))]
    result = result.at[tuple(index_at)].set(smallest)
    longest = dims.index(max(dims))
    index_at[longest] = (index_at[longest] + 1) % dims[longest]
    return result.at[tuple(index_at)].set(top_value)


def steps_of(own_key, shape, cuts, least, top_value):
    factor_of = 1.0
    for axis_at, blocks in cuts:
        heights = jax.random.uniform(jax.random.fold_in(jax.random.fold_in(own_key, 6), axis_at), (blocks,), jnp.float32, least / len(cuts), top_value / len(cuts))
        factor_of = factor_of * jnp.repeat(jnp.exp(heights), shape[axis_at] // blocks).reshape((-1,) + (1,) * (len(shape) - 1 - axis_at))
    return factor_of


def bell_draw(key, extent, deviation, bound, split=(), held_as=jnp.bfloat16):
    drawn = deviation * jax.random.normal(key, extent, jnp.float32)
    if split:
        drawn = drawn * steps_of(key, extent, split, -0.22, 0.18)
    return jnp.clip(drawn, -bound, bound).astype(held_as)


def setup_inputs(seed: int = 0) -> dict:
    streams_of = jax.random.split(jax.random.key(seed), 4)
    profiles = bell_draw(streams_of[0], (BATCHES, 2, R, F), 1.0, 6.0, ((0, 4), (2, 8)))
    range_walk = plant(jax.random.randint(streams_of[1], (F,), -WALK, WALK + 1), jax.random.fold_in(streams_of[1], 1), -WALK, WALK).astype(jnp.int32)
    band_order = jax.random.permutation(streams_of[2], BANDS).astype(jnp.int32)
    return dict(profiles=profiles, range_walk=range_walk, band_order=band_order)


def fourier_tables(length):
    counter = jnp.arange(length, dtype=jnp.int32)
    phases = (counter[:, None] * counter[None, :]) % length
    angles = phases.astype(jnp.float32) * (2.0 * math.pi / length)
    return jnp.cos(angles).astype(jnp.bfloat16), jnp.sin(angles).astype(jnp.bfloat16)


def batch_powers(block, cosine, sine_table):
    count = block.shape[0]
    delays = block.shape[2]
    bins = block.shape[3]
    stacked = block.reshape(count * 2 * delays, bins)
    first = jnp.dot(stacked, cosine, preferred_element_type=jnp.float32).reshape(count, 2, delays, bins)
    second = jnp.dot(stacked, sine_table, preferred_element_type=jnp.float32).reshape(count, 2, delays, bins)
    real_part = first[:, 0] + second[:, 1]
    imag_part = first[:, 1] - second[:, 0]
    return real_part * real_part + imag_part * imag_part


def reference(profiles, range_walk, band_order):
    cosine, sine_table = fourier_tables(F)

    def accumulate(running, inputs):
        block, batch = inputs
        powers = batch_powers(block[None], cosine, sine_table)[0]
        offsets = (range_walk * batch) // BATCHES
        padded = jnp.pad(powers, ((WALK, WALK), (0, 0)))
        lookup = jnp.arange(R, dtype=jnp.int32)[:, None] + offsets[None, :] + WALK
        aligned = jnp.take_along_axis(padded, lookup.astype(jnp.int32), axis=0)
        return running + aligned, jnp.zeros((), jnp.float32)

    start = jnp.zeros((R, F), jnp.float32)
    scanned = lax.scan(accumulate, start, (profiles, jnp.arange(BATCHES, dtype=jnp.int32)))
    power_map = (scanned[0] * (1.0 / (BATCHES * F))).T
    ordered = jnp.take(power_map.reshape(BANDS, BAND_ROWS, R), band_order, axis=0)
    return ordered.reshape(F, R)
```

```python
import functools
import math

import jax
import jax.numpy as jnp
import numpy as np
from jax import lax
from jax.experimental import pallas as pl
from jax.experimental.pallas import tpu as pltpu
from jax.sharding import PartitionSpec as P

WALK = 32
LANES = 128
TILE = 16
RADIX = 4


def rotation(rows, pulses, length):
    phases = (np.asarray(rows)[..., None] * np.arange(pulses)) % length
    angles = phases * (2.0 * math.pi / length)
    return np.cos(angles).astype(np.float32), np.sin(angles).astype(np.float32)


def quarter_sums(x_ref, at, short):
    re = [x_ref[at, 0, :, q * short:(q + 1) * short].astype(jnp.float32) for q in range(RADIX)]
    im = [x_ref[at, 1, :, q * short:(q + 1) * short].astype(jnp.float32) for q in range(RADIX)]
    are, aim, bre, bim = re[0] + re[2], im[0] + im[2], re[0] - re[2], im[0] - im[2]
    cre, cim, dre, dim = re[1] + re[3], im[1] + im[3], re[1] - re[3], im[1] - im[3]
    return (
        (are + cre, aim + cim),
        (bre + dim, bim - dre),
        (are - cre, aim - cim),
        (bre - dim, bim + dre),
    )


def power_kernel(
    batch_count, total_batches, per_band, scale, joined,
    order_ref, x_ref, walk_ref, turns, *refs,
):
    *outs, table, packed, own_sum, rim_sum, walks = refs
    step = pl.program_id(0)
    short = x_ref.shape[3] // RADIX
    bins = table.shape[1]
    base_rows = max(per_band, TILE)
    bands_at = RADIX * base_rows

    @pl.when(step == 0)
    def _():
        own_sum[...] = jnp.zeros_like(own_sum)
        rim_sum[...] = jnp.zeros_like(rim_sum)
        row = lax.broadcasted_iota(jnp.int32, (TILE, short), 0) // min(per_band, TILE)

        @pl.loop(0, bins // TILE)
        def _(tile):
            start = pl.multiple_of(tile * TILE, TILE)
            first = start // per_band
            inside = pl.multiple_of(start % per_band, TILE) if per_band > TILE else 0
            vc = turns[0, pl.ds(bands_at + order_ref[first], 1), :]
            vs = turns[1, pl.ds(bands_at + order_ref[first], 1), :]
            for extra in range(1, max(1, TILE // per_band)):
                band = order_ref[first + extra]
                vc = jnp.where(row == extra, turns[0, pl.ds(bands_at + band, 1), :], vc)
                vs = jnp.where(row == extra, turns[1, pl.ds(bands_at + band, 1), :], vs)
            for r in range(RADIX):
                if joined:
                    at = order_ref[first] * (per_band * RADIX) + inside * RADIX + r
                    walks[r, pl.ds(start, TILE), :] = walk_ref[pl.ds(at, TILE, stride=RADIX), :]
                else:
                    walks[r, pl.ds(start, TILE), :] = walk_ref[r, pl.ds(start, TILE), :]
                bc = turns[0, pl.ds(r * base_rows + inside, TILE), :]
                bs = turns[1, pl.ds(r * base_rows + inside, TILE), :]
                table[r, pl.ds(start, TILE), :short] = (bc * vc - bs * vs).astype(jnp.bfloat16)
                table[r, pl.ds(start, TILE), short:] = (bs * vc + bc * vs).astype(jnp.bfloat16)

    each = x_ref.shape[0]
    batch = lax.axis_index("slow") * batch_count + step * each
    lane = lax.broadcasted_iota(jnp.int32, (bins, LANES), 1)
    for at in range(each):
        top, low = 2 * LANES * at, 2 * LANES * at + LANES
        for r, parts in enumerate(quarter_sums(x_ref, at, short)):
            yre, yim = (part.astype(jnp.bfloat16) for part in parts)
            packed[r, top:low, :short] = yre
            packed[r, top:low, short:] = yim
            packed[r, low:low + LANES, :short] = yim
            packed[r, low:low + LANES, short:] = -yre

    def align(r, spec):
        own_add, rim_add = 0.0, 0.0
        for at in range(each):
            re = spec[:, 2 * LANES * at:2 * LANES * at + LANES]
            im = spec[:, 2 * LANES * at + LANES:2 * LANES * (at + 1)]
            power = re * re + im * im
            moved = walks[r] * (batch + at)
            if power_of_two(total_batches):
                offset = lax.shift_right_arithmetic(moved, total_batches.bit_length() - 1)
            else:
                offset = jnp.floor_divide(moved, total_batches)
            source = lane + offset
            wrapped = source & (LANES - 1)
            value = jnp.take_along_axis(power, wrapped, axis=1, mode="promise_in_bounds")
            inside = source == wrapped
            own_add += jnp.where(inside, value, 0.0)
            rim_add += jnp.where(inside, 0.0, value)
        own_sum[r] += own_add
        rim_sum[r] += rim_add

    pending = None
    for r in range(RADIX):
        spec = lax.dot_general(
            table[r], packed[r], (((1,), (1,)), ((), ())), preferred_element_type=jnp.float32
        )
        if pending is not None:
            align(r - 1, pending)
        pending = spec
    align(RADIX - 1, pending)

    @pl.when(step == pl.num_programs(0) - 1)
    def _():
        if joined:
            out_ref = outs[0]
            band_rows = per_band * RADIX
            half = band_rows // 2

            @pl.loop(0, bins // per_band)
            def _(block):
                rows = pl.ds(pl.multiple_of(block * per_band, per_band), per_band)
                for r in range(RADIX):
                    out_ref[block, pl.ds(r, per_band, stride=RADIX), :] = rim_sum[r, rows, :] * scale
                low, high = out_ref[block, :half, :], out_ref[block, half:band_rows, :]
                out_ref[block, band_rows:, :] = low + pltpu.roll(high, LANES // 2, 1)
                for r in range(RADIX):
                    out_ref[block, pl.ds(r, per_band, stride=RADIX), :] = own_sum[r, rows, :] * scale
        else:
            for r in range(RADIX):
                outs[0][pl.ds(r, bins, stride=RADIX), :] = own_sum[r] * scale
                outs[1][pl.ds(r, bins, stride=RADIX), :] = rim_sum[r] * scale


def aligned_power(profiles, range_walk, band_order, total_batches, joined):
    batch_count, _, delays, pulses = profiles.shape
    band_count = band_order.shape[0]
    band_rows = pulses // band_count
    per_band = band_rows // RADIX
    bins, short = pulses // RADIX, pulses // RADIX
    scale = 1.0 / (total_batches * pulses)
    if delays < LANES:
        profiles = jnp.pad(profiles, ((0, 0), (0, 0), (0, LANES - delays), (0, 0)))
    if joined:
        walks = jnp.broadcast_to(range_walk[:, None], (pulses, LANES))
    else:
        picked = band_order[:, None, None] == jnp.arange(band_count, dtype=jnp.int32)[None, :, None]
        walks = jnp.sum(jnp.where(picked, range_walk.reshape(1, band_count, band_rows), 0), axis=1)
        walks = jnp.broadcast_to(walks.reshape(bins, RADIX).T[:, :, None], (RADIX, bins, LANES))
    each = 2 if batch_count % 2 == 0 else 1
    inner = np.arange(max(per_band, TILE)) % per_band
    base = (RADIX * inner[None, :] + np.arange(RADIX)[:, None]).reshape(-1)
    band = np.arange(band_count) * band_rows
    turns = np.stack(rotation(np.concatenate([base, band]), short, pulses))
    whole = lambda shape: pl.BlockSpec(shape, lambda g, order: (0,) * len(shape))
    if joined:
        shapes = ((band_count, band_rows + band_rows // 2, LANES),)
    else:
        shapes = ((pulses, LANES),) * 2
    return pl.pallas_call(
        functools.partial(power_kernel, batch_count, total_batches, per_band, scale, joined),
        out_shape=[jax.ShapeDtypeStruct(shape, jnp.float32) for shape in shapes],
        grid_spec=pltpu.PrefetchScalarGridSpec(
            num_scalar_prefetch=1,
            grid=(batch_count // each,),
            in_specs=[
                pl.BlockSpec((each, 2, LANES, pulses), lambda g, order: (g, 0, 0, 0)),
                whole(walks.shape),
                whole(turns.shape),
            ],
            out_specs=[whole(shape) for shape in shapes],
            scratch_shapes=[
                pltpu.VMEM((RADIX, bins, 2 * short), jnp.bfloat16),
                pltpu.VMEM((RADIX, 2 * LANES * each, 2 * short), jnp.bfloat16),
                pltpu.VMEM((RADIX, bins, LANES), jnp.float32),
                pltpu.VMEM((RADIX, bins, LANES), jnp.float32),
                pltpu.VMEM((RADIX, bins, LANES), jnp.int32),
            ],
        ),
        compiler_params=pltpu.CompilerParams(
            dimension_semantics=("arbitrary",), vmem_limit_bytes=48 << 20
        ),
    )(band_order, profiles, walks, jnp.asarray(turns))


MESH = pl.DeviceIdType.MESH


def bit_of(value, k):
    return lax.rem(lax.div(value, 1 << k), 2)


def flipped(value, mask):
    result = value
    for k in range(mask.bit_length()):
        if mask >> k & 1:
            result = result + (1 << k) * (1 - 2 * bit_of(value, k))
    return result


def regroup_kernel(dop_count, slow_count, data, out_ref, *refs):
    levels = slow_count.bit_length() - 1
    kept, arrived = refs[:levels], refs[levels:2 * levels]
    landed, send_sem, recv_sem = refs[2 * levels:]
    dop, slow = lax.axis_index("dop"), lax.axis_index("slow")
    band_rows = out_ref.shape[0]
    partners = [(dop, flipped(slow, 1 << k)) for k in range(levels)]
    partners += [(flipped(dop, j), slow) for j in range(1, dop_count)]

    barrier = pltpu.get_barrier_semaphore()
    for partner in partners:
        pl.semaphore_signal(barrier, inc=1, device_id=partner, device_id_type=MESH)
    pl.semaphore_wait(barrier, len(partners))

    order = list(range(dop_count - 1, -1, -1))
    copies = {}

    def send(level, j, source, target, device):
        copies[level, j] = pltpu.make_async_remote_copy(
            src_ref=source, dst_ref=target,
            send_sem=send_sem.at[level, j], recv_sem=recv_sem.at[level, j],
            device_id=device, device_id_type=MESH,
        )
        copies[level, j].start()

    for j in order:
        send(0, j, data.at[flipped(dop, j), :, 1 - bit_of(slow, 0)], arrived[0].at[j], partners[0])
    for level in range(levels):
        for j in order:
            copies[level, j].wait_recv()
            bit = bit_of(slow, level)
            held = data[flipped(dop, j), :, bit] if level == 0 else kept[level - 1][j, :, bit]
            total = held + arrived[level][j]
            if level < levels - 1:
                kept[level][j] = total.reshape(kept[level].shape[1:])
                send(
                    level + 1, j, kept[level].at[j, :, 1 - bit_of(slow, level + 1)],
                    arrived[level + 1].at[j], partners[level + 1],
                )
            elif j:
                kept[level][j] = total[0]
                send(levels, j, kept[level].at[j], landed.at[j], (flipped(dop, j), slow))
            else:
                landed[0] = total[0]
    for j in order[:-1]:
        copies[levels, j].wait_recv()

    half = band_rows // 2
    lane = lax.broadcasted_iota(jnp.int32, (half, LANES), 1)
    for e in range(dop_count):
        main = landed[flipped(dop, e), :band_rows, :]
        low = jnp.zeros((half, LANES), jnp.float32)
        high = low
        for source, mine in ((e - 1, lane < WALK), (e + 1, lane >= LANES - WALK)):
            if 0 <= source < dop_count:
                rim = landed[flipped(dop, source), band_rows:, :]
                low += jnp.where(mine, rim, 0.0)
                high += jnp.where(mine, pltpu.roll(rim, LANES // 2, 1), 0.0)
        out_ref[:half, e * LANES:(e + 1) * LANES] = main[:half] + low
        out_ref[half:, e * LANES:(e + 1) * LANES] = main[half:] + high
    for copy in copies.values():
        copy.wait_send()


def regroup(blocks, dop_count, slow_count):
    rows = blocks.shape[1]
    band_rows = rows // 3 * 2
    levels = slow_count.bit_length() - 1
    kept, arrived = [], []
    count = slow_count
    for level in range(levels):
        count //= 2
        pair = (count // 2, 2) if count > 1 else ()
        kept.append(pltpu.VMEM((dop_count, *pair, rows, LANES), jnp.float32))
        arrived.append(pltpu.VMEM((dop_count, count, rows, LANES), jnp.float32))
    return pl.pallas_call(
        functools.partial(regroup_kernel, dop_count, slow_count),
        out_shape=jax.ShapeDtypeStruct((band_rows, dop_count * LANES), jnp.float32),
        in_specs=[pl.BlockSpec(memory_space=pltpu.VMEM)],
        out_specs=pl.BlockSpec(memory_space=pltpu.VMEM),
        scratch_shapes=[
            *kept, *arrived,
            pltpu.VMEM((dop_count, rows, LANES), jnp.float32),
            pltpu.SemaphoreType.DMA((levels + 1, dop_count)),
            pltpu.SemaphoreType.DMA((levels + 1, dop_count)),
        ],
        compiler_params=pltpu.CompilerParams(
            collective_id=0, has_side_effects=True, vmem_limit_bytes=32 << 20
        ),
    )(blocks.reshape(dop_count, slow_count // 2, 2, rows, LANES))


def power_of_two(count):
    return count & (count - 1) == 0


def neighbours(value, steps):
    count = lax.axis_size("dop")
    pairs = [(source, source + steps) for source in range(count) if 0 <= source + steps < count]
    return lax.ppermute(value, "dop", pairs)


def exchange(own, rim, delays):
    dop_count, slow_count = lax.axis_size("dop"), lax.axis_size("slow")
    rows = own.shape[0] // (dop_count * slow_count)
    after = rim[:, :WALK] if delays == LANES else own[:, delays:delays + WALK]
    from_below = neighbours(after, 1)
    from_above = neighbours(rim[:, LANES - WALK:], -1)
    own = own[:, :delays].at[:, :WALK].add(from_below)
    own = own.at[:, delays - WALK:].add(from_above)
    grouped = own.reshape(dop_count, slow_count, rows, delays)
    summed = lax.psum_scatter(grouped, "slow", scatter_dimension=1, tiled=False)
    gathered = lax.all_to_all(summed, "dop", split_axis=0, concat_axis=0, tiled=True)
    return gathered.transpose(1, 0, 2).reshape(rows, dop_count * delays)


FAN = 8
SUB = 8
PIECE = 32
PAIR = 2


def fan_table(pulses):
    short = pulses // FAN
    rows = (FAN * np.arange(short)[None, :] + np.arange(FAN)[:, None])[..., None]
    phases = (rows * np.arange(short)) % pulses
    angles = phases.astype(np.float32) * np.float32(2.0 * math.pi / pulses)
    return jnp.asarray(np.concatenate([np.cos(angles), np.sin(angles)], axis=2), jnp.bfloat16)


def turned(re, im):
    half = math.sqrt(0.5)
    are = [re[q] + re[q + 4] for q in range(4)]
    aim = [im[q] + im[q + 4] for q in range(4)]
    bre = [re[q] - re[q + 4] for q in range(4)]
    bim = [im[q] - im[q + 4] for q in range(4)]
    out = [None] * FAN
    c0, c1, c2, c3 = are[0] + are[2], are[0] - are[2], are[1] + are[3], are[1] - are[3]
    s0, s1, s2, s3 = aim[0] + aim[2], aim[0] - aim[2], aim[1] + aim[3], aim[1] - aim[3]
    out[0], out[4] = (c0 + c2, s0 + s2), (c0 - c2, s0 - s2)
    out[2], out[6] = (c1 + s3, s1 - c3), (c1 - s3, s1 + c3)
    d0re, d0im, d1re, d1im = bre[0] + bim[2], bim[0] - bre[2], bre[0] - bim[2], bim[0] + bre[2]
    p1, m1 = bre[1] + bim[1], bim[1] - bre[1]
    p3, m3 = bre[3] + bim[3], bim[3] - bre[3]
    e2re, e2im = (p1 + m3) * half, (m1 - p3) * half
    e3re, e3im = (p1 - m3) * half, (m1 + p3) * half
    out[1], out[5] = (d0re + e2re, d0im + e2im), (d0re - e2re, d0im - e2im)
    out[3], out[7] = (d1re + e3im, d1im - e3re), (d1re - e3im, d1im + e3re)
    return out


def fused_body(
    accs, dop_count, total_batches, scale,
    x_hbm, table_hbm, walk_ref, order_ref, out_ref,
    x_buf, table, minus, y_buf, spun, walks, own, rim, stage,
    held, near, passed, across, last, landed,
    x_sem, table_sem, near_send, near_recv, across_send, across_recv, land_send, land_recv,
):
    batches, _, delays, pulses = x_buf.shape
    short = pulses // FAN
    pairs = batches // PAIR
    bands = order_ref.shape[0]
    dop, slow = lax.axis_index("dop"), lax.axis_index("slow")
    core, side = lax.rem(slow, 2), lax.div(slow, 2)
    core_peer, side_peer = (dop, flipped(slow, 1)), (dop, flipped(slow, 2))
    partners = [core_peer, side_peer] + [(flipped(dop, j), slow) for j in range(1, dop_count)]
    groups = LANES // WALK
    units = FAN + FAN // groups

    loads = [pltpu.make_async_copy(x_hbm.at[g], x_buf.at[g], x_sem.at[g]) for g in range(batches)]
    for load in loads:
        load.start()
    table_loads = [
        pltpu.make_async_copy(table_hbm.at[r], table.at[r], table_sem.at[r]) for r in range(FAN)
    ]
    for load in table_loads:
        load.start()

    barrier = pltpu.get_barrier_semaphore()
    for partner in partners:
        pl.semaphore_signal(barrier, inc=1, device_id=partner, device_id_type=MESH)

    for a in range(pulses // LANES):
        row = jnp.broadcast_to(walk_ref[a:a + 1, :], (LANES, LANES))
        spun[a * LANES:(a + 1) * LANES, :] = row.T
    for r in range(FAN):
        walks[r] = spun[pl.ds(r, short, stride=FAN), :].reshape(-1, SUB, LANES)

    def spread(g):
        @pl.loop(0, delays // 16)
        def _(block):
            at = pl.ds(pl.multiple_of(block * 16, 16), 16)
            to = pl.ds(pl.multiple_of((g % PAIR) * delays + block * 16, 16), 16)
            for lane in range(0, short, LANES):
                parts = [
                    [
                        x_buf[g, c, at, q * short + lane:q * short + lane + LANES].astype(jnp.float32)
                        for q in range(FAN)
                    ]
                    for c in range(2)
                ]
                for r, (re, im) in enumerate(turned(*parts)):
                    y_buf[r, g // PAIR, to, lane:lane + LANES] = re.astype(jnp.bfloat16)
                    y_buf[r, g // PAIR, to, short + lane:short + lane + LANES] = im.astype(jnp.bfloat16)

    for g in range(batches):
        loads[g].wait()
        spread(g)

    lane = lax.broadcasted_iota(jnp.int32, (PIECE, LANES), 1)
    thin = lax.broadcasted_iota(jnp.int32, (SUB, LANES), 1)
    shift = total_batches.bit_length() - 1
    lanes = lane * total_batches
    first_batch = slow * batches
    pieces = short // PIECE

    def align(r, half, piece, specs):
        at = slice(piece * PIECE // SUB, (piece + 1) * PIECE // SUB)
        walk = walks[r, at].reshape(PIECE, LANES)
        own_add, rim_add = None, None
        for q, (re, im) in enumerate(specs):
            power = re * re + im * im
            for b in range(PAIR):
                batch = first_batch + (2 * half + q) * PAIR + b
                source = lax.shift_right_arithmetic(lanes + walk * batch, shift)
                wrapped = source & (LANES - 1)
                value = jnp.take_along_axis(
                    power[:, b * LANES:(b + 1) * LANES], wrapped, axis=1, mode="promise_in_bounds"
                )
                inside = source == wrapped
                kept, spilled = jnp.where(inside, value, 0.0), jnp.where(inside, 0.0, value)
                own_add = kept if own_add is None else own_add + kept
                rim_add = spilled if rim_add is None else rim_add + spilled
        if half:
            own_add += own[r % 2, at].reshape(PIECE, LANES)
            rim_add += rim[r % 2, at].reshape(PIECE, LANES)
        own[r % 2, at] = own_add.reshape(-1, SUB, LANES)
        rim[r % 2, at] = rim_add.reshape(-1, SUB, LANES)

    def slot(band):
        owner_dop, owner_slow = divmod(band, 4)
        return owner_slow % 2, owner_dop, owner_slow // 2

    copies = {}

    def send(key, source, target, sent, received, device):
        copies[key] = pltpu.make_async_remote_copy(
            src_ref=source, dst_ref=target, send_sem=sent, recv_sem=received,
            device_id=device, device_id_type=MESH,
        )
        copies[key].start()

    def send_near(u):
        send(("near", u), held.at[u, 1 - core], near.at[u], near_send.at[u], near_recv.at[u], core_peer)

    def send_across(u):
        copies["near", u].wait_recv()
        for d in range(dop_count):
            passed[u, d] = held[u, core, d, 1 - side] + near[u, d, 1 - side]
        send(
            ("across", u), passed.at[u], across.at[u], across_send.at[u], across_recv.at[u], side_peer
        )

    def send_home(u):
        copies["across", u].wait_recv()
        for j in range(dop_count - 1, -1, -1):
            d = flipped(dop, j)
            total = held[u, core, d, side] + near[u, d, side] + across[u, d]
            if j:
                last[u, j] = total
                send(
                    ("home", u, j), last.at[u, j], landed.at[u, j],
                    land_send.at[u, j], land_recv.at[u, j], (d, slow),
                )
            else:
                landed[u, 0] = total

    def arrive(u):
        for j in range(dop_count - 1, 0, -1):
            copies["home", u, j].wait_recv()

    def unit_of(r):
        return r + r // groups

    def put(r):
        for e in range(dop_count):
            stage[e, pl.ds(r, SUB, stride=FAN), :] = landed[unit_of(r), flipped(dop, e)]

    def put_rim(h):
        mine = order_ref[dop * 4 + slow]
        u = h * (groups + 1) + groups
        for k in range(groups):
            r = h * groups + k
            walk = walks[r, mine]
            after = jnp.logical_and(walk < 0, thin < WALK)
            before = jnp.logical_and(walk > 0, thin >= LANES - WALK)
            for e in range(dop_count):
                add = 0.0
                for source, mask, move in ((e - 1, after, -k * WALK), (e + 1, before, LANES - WALK - k * WALK)):
                    if 0 <= source < dop_count:
                        value = landed[u, flipped(dop, source)]
                        if move % LANES:
                            value = pltpu.roll(value, move % LANES, 1)
                        add = add + jnp.where(mask, value, 0.0)
                at = (e, pl.ds(r, SUB, stride=FAN), slice(None))
                stage[at] = stage[at] + add

    def pack(r):
        u = unit_of(r)
        k = r % groups
        for band in range(bands):
            source = order_ref[band]
            c, d, s = slot(band)
            held[u, c, d, s] = own[r % 2, source] * scale
            edge = rim[r % 2, source] * scale
            left = pltpu.roll(edge, k * WALK, 1) if k else edge
            right = pltpu.roll(edge, (k * WALK + WALK) % LANES, 1) if (k + 1) % groups else edge
            mask = jnp.logical_and(thin >= k * WALK, thin < (k + 1) * WALK)
            value = jnp.where(mask, left + right, 0.0)
            v = (r // groups) * (groups + 1) + groups
            held[v, c, d, s] = value if k == 0 else held[v, c, d, s] + value

    for r in range(FAN):
        table_loads[r].wait()
        minus[...] = -table[r, :, :short]
        for half in range(pairs // 2):
            for q in range(2):
                p = 2 * half + q
                re_accs, im_accs = accs[q][half % 2]
                pltpu.matmul_push_rhs(y_buf[r, p, :, :short], 0, q, transpose=True)
                pltpu.matmul_push_rhs(y_buf[r, p, :, short:], 1, q, transpose=True)
                for piece in range(pieces):
                    rows = slice(piece * PIECE, (piece + 1) * PIECE)
                    pltpu.matmul_acc_lhs(
                        re_accs[piece], table[r, rows, :short], load_staged_rhs=0 if piece == 0 else None
                    )
                    pltpu.matmul_acc_lhs(im_accs[piece], table[r, rows, short:])
                for piece in range(pieces):
                    rows = slice(piece * PIECE, (piece + 1) * PIECE)
                    pltpu.matmul_acc_lhs(
                        re_accs[piece], table[r, rows, short:], load_staged_rhs=1 if piece == 0 else None
                    )
                    pltpu.matmul_acc_lhs(im_accs[piece], minus[rows, :])
            for piece in range(pieces):
                specs = []
                for q in range(2):
                    re_accs, im_accs = accs[q][half % 2]
                    specs.append((pltpu.matmul_pop(re_accs[piece]), pltpu.matmul_pop(im_accs[piece])))
                align(r, half, piece, specs)
        pack(r)
        if r == 0:
            pl.semaphore_wait(barrier, len(partners))
        send_near(unit_of(r))
        if r % groups == groups - 1:
            send_near(unit_of(r) + 1)
        if r >= 1:
            send_across(unit_of(r - 1))
            if (r - 1) % groups == groups - 1:
                send_across(unit_of(r - 1) + 1)

    for u in range(unit_of(FAN - 1), units):
        send_across(u)
    for u in range(units):
        send_home(u)
    for h in range(FAN // groups):
        for k in range(groups):
            r = h * groups + k
            arrive(unit_of(r))
            put(r)
        arrive(unit_of(r) + 1)
        put_rim(h)
    for e in range(dop_count):
        out_ref[:, e * LANES:(e + 1) * LANES] = stage[e]
    for copy in copies.values():
        copy.wait_send()


def fused_kernel(dop_count, total_batches, scale, x_hbm, *refs):
    pieces = x_hbm.shape[3] // (FAN * PIECE)

    def sums(q):
        return tuple(pltpu.ACC(q)((PIECE, 2 * LANES), jnp.float32) for _ in range(pieces))

    def run(accs):
        fused_body(accs, dop_count, total_batches, scale, x_hbm, *refs)

    pl.run_scoped(run, tuple(tuple((sums(q), sums(q)) for _ in range(2)) for q in range(2)))


def fused(profiles, range_walk, band_order, dop_count, total_batches):
    batches, _, delays, pulses = profiles.shape
    bands = band_order.shape[0]
    short = pulses // FAN
    units = FAN + FAN // (LANES // WALK)
    vmem = pl.BlockSpec(memory_space=pltpu.VMEM)
    blocks = (SUB, LANES)
    f32 = jnp.float32
    return pl.pallas_call(
        functools.partial(fused_kernel, dop_count, total_batches, 1.0 / (total_batches * pulses)),
        out_shape=jax.ShapeDtypeStruct((pulses // bands, dop_count * delays), f32),
        in_specs=[
            pl.BlockSpec(memory_space=pl.ANY), pl.BlockSpec(memory_space=pl.ANY),
            vmem, pl.BlockSpec(memory_space=pltpu.SMEM),
        ],
        out_specs=vmem,
        scratch_shapes=[
            pltpu.VMEM(profiles.shape, jnp.bfloat16),
            pltpu.VMEM((FAN, short, 2 * short), jnp.bfloat16),
            pltpu.VMEM((short, short), jnp.bfloat16),
            pltpu.VMEM((FAN, batches // PAIR, PAIR * delays, 2 * short), jnp.bfloat16),
            pltpu.VMEM((pulses, LANES), jnp.int32),
            pltpu.VMEM((FAN, short // SUB, SUB, LANES), jnp.int32),
            pltpu.VMEM((2, short // SUB, SUB, LANES), f32),
            pltpu.VMEM((2, short // SUB, SUB, LANES), f32),
            pltpu.VMEM((dop_count, pulses // bands, LANES), f32),
            pltpu.VMEM((units, 2, dop_count, 2, *blocks), f32),
            pltpu.VMEM((units, dop_count, 2, *blocks), f32),
            pltpu.VMEM((units, dop_count, *blocks), f32),
            pltpu.VMEM((units, dop_count, *blocks), f32),
            pltpu.VMEM((units, dop_count, *blocks), f32),
            pltpu.VMEM((units, dop_count, *blocks), f32),
            pltpu.SemaphoreType.DMA((batches,)),
            pltpu.SemaphoreType.DMA((FAN,)),
            pltpu.SemaphoreType.DMA((units,)),
            pltpu.SemaphoreType.DMA((units,)),
            pltpu.SemaphoreType.DMA((units,)),
            pltpu.SemaphoreType.DMA((units,)),
            pltpu.SemaphoreType.DMA((units, dop_count)),
            pltpu.SemaphoreType.DMA((units, dop_count)),
        ],
        compiler_params=pltpu.CompilerParams(
            collective_id=0, has_side_effects=True, vmem_limit_bytes=60 << 20
        ),
    )(profiles, fan_table(pulses), range_walk.reshape(pulses // LANES, LANES), band_order)


def fits(profiles, band_order, dop_count, slow_count, total_batches):
    batches, _, delays, pulses = profiles.shape
    return (
        delays == LANES and pulses == 2 * LANES * FAN and batches % (2 * PAIR) == 0
        and pulses == band_order.shape[0] * SUB * FAN and band_order.shape[0] == dop_count * slow_count
        and slow_count == 4 and dop_count > 1 and power_of_two(dop_count) and power_of_two(total_batches)
    )


def on_device(profiles, range_walk, band_order):
    total_batches = profiles.shape[0] * lax.axis_size("slow")
    delays = profiles.shape[2]
    dop_count, slow_count = lax.axis_size("dop"), lax.axis_size("slow")
    if fits(profiles, band_order, dop_count, slow_count, total_batches):
        return fused(profiles, range_walk, band_order, dop_count, total_batches)
    per_band = profiles.shape[3] // (dop_count * slow_count * RADIX)
    joined = (
        delays == LANES and per_band % TILE == 0 and slow_count > 1
        and power_of_two(dop_count) and power_of_two(slow_count)
    )
    sums = aligned_power(profiles, range_walk, band_order, total_batches, joined)
    if joined:
        return regroup(sums[0], dop_count, slow_count)
    return exchange(*sums, delays)


def solution(mesh):
    placed = (P("slow", None, "dop", None), P(), P())
    return jax.shard_map(
        on_device, mesh=mesh, in_specs=placed, out_specs=P(("dop", "slow"), None), check_vma=False
    )
```

```python
import functools
import math

import jax
import jax.numpy as jnp
import numpy as np
from jax import lax
from jax.experimental import pallas as pl
from jax.experimental.pallas import tpu as pltpu
from jax.sharding import PartitionSpec as P

WALK = 32
LANES = 128
TILE = 16
RADIX = 4


def rotation(rows, pulses, length):
    phases = (np.asarray(rows)[..., None] * np.arange(pulses)) % length
    angles = phases * (2.0 * math.pi / length)
    return np.cos(angles).astype(np.float32), np.sin(angles).astype(np.float32)


def quarter_sums(x_ref, at, short):
    re = [x_ref[at, 0, :, q * short:(q + 1) * short].astype(jnp.float32) for q in range(RADIX)]
    im = [x_ref[at, 1, :, q * short:(q + 1) * short].astype(jnp.float32) for q in range(RADIX)]
    are, aim, bre, bim = re[0] + re[2], im[0] + im[2], re[0] - re[2], im[0] - im[2]
    cre, cim, dre, dim = re[1] + re[3], im[1] + im[3], re[1] - re[3], im[1] - im[3]
    return (
        (are + cre, aim + cim),
        (bre + dim, bim - dre),
        (are - cre, aim - cim),
        (bre - dim, bim + dre),
    )


def power_kernel(
    batch_count, total_batches, per_band, scale, joined,
    order_ref, x_ref, walk_ref, turns, *refs,
):
    *outs, table, packed, own_sum, rim_sum, walks = refs
    step = pl.program_id(0)
    short = x_ref.shape[3] // RADIX
    bins = table.shape[1]
    base_rows = max(per_band, TILE)
    bands_at = RADIX * base_rows

    @pl.when(step == 0)
    def _():
        own_sum[...] = jnp.zeros_like(own_sum)
        rim_sum[...] = jnp.zeros_like(rim_sum)
        row = lax.broadcasted_iota(jnp.int32, (TILE, short), 0) // min(per_band, TILE)

        @pl.loop(0, bins // TILE)
        def _(tile):
            start = pl.multiple_of(tile * TILE, TILE)
            first = start // per_band
            inside = pl.multiple_of(start % per_band, TILE) if per_band > TILE else 0
            vc = turns[0, pl.ds(bands_at + order_ref[first], 1), :]
            vs = turns[1, pl.ds(bands_at + order_ref[first], 1), :]
            for extra in range(1, max(1, TILE // per_band)):
                band = order_ref[first + extra]
                vc = jnp.where(row == extra, turns[0, pl.ds(bands_at + band, 1), :], vc)
                vs = jnp.where(row == extra, turns[1, pl.ds(bands_at + band, 1), :], vs)
            for r in range(RADIX):
                if joined:
                    at = order_ref[first] * (per_band * RADIX) + inside * RADIX + r
                    walks[r, pl.ds(start, TILE), :] = walk_ref[pl.ds(at, TILE, stride=RADIX), :]
                else:
                    walks[r, pl.ds(start, TILE), :] = walk_ref[r, pl.ds(start, TILE), :]
                bc = turns[0, pl.ds(r * base_rows + inside, TILE), :]
                bs = turns[1, pl.ds(r * base_rows + inside, TILE), :]
                table[r, pl.ds(start, TILE), :short] = (bc * vc - bs * vs).astype(jnp.bfloat16)
                table[r, pl.ds(start, TILE), short:] = (bs * vc + bc * vs).astype(jnp.bfloat16)

    each = x_ref.shape[0]
    batch = lax.axis_index("slow") * batch_count + step * each
    lane = lax.broadcasted_iota(jnp.int32, (bins, LANES), 1)
    for at in range(each):
        top, low = 2 * LANES * at, 2 * LANES * at + LANES
        for r, parts in enumerate(quarter_sums(x_ref, at, short)):
            yre, yim = (part.astype(jnp.bfloat16) for part in parts)
            packed[r, top:low, :short] = yre
            packed[r, top:low, short:] = yim
            packed[r, low:low + LANES, :short] = yim
            packed[r, low:low + LANES, short:] = -yre

    def align(r, spec):
        own_add, rim_add = 0.0, 0.0
        for at in range(each):
            re = spec[:, 2 * LANES * at:2 * LANES * at + LANES]
            im = spec[:, 2 * LANES * at + LANES:2 * LANES * (at + 1)]
            power = re * re + im * im
            moved = walks[r] * (batch + at)
            if power_of_two(total_batches):
                offset = lax.shift_right_arithmetic(moved, total_batches.bit_length() - 1)
            else:
                offset = jnp.floor_divide(moved, total_batches)
            source = lane + offset
            wrapped = source & (LANES - 1)
            value = jnp.take_along_axis(power, wrapped, axis=1, mode="promise_in_bounds")
            inside = source == wrapped
            own_add += jnp.where(inside, value, 0.0)
            rim_add += jnp.where(inside, 0.0, value)
        own_sum[r] += own_add
        rim_sum[r] += rim_add

    pending = None
    for r in range(RADIX):
        spec = lax.dot_general(
            table[r], packed[r], (((1,), (1,)), ((), ())), preferred_element_type=jnp.float32
        )
        if pending is not None:
            align(r - 1, pending)
        pending = spec
    align(RADIX - 1, pending)

    @pl.when(step == pl.num_programs(0) - 1)
    def _():
        if joined:
            out_ref = outs[0]
            band_rows = per_band * RADIX
            half = band_rows // 2

            @pl.loop(0, bins // per_band)
            def _(block):
                rows = pl.ds(pl.multiple_of(block * per_band, per_band), per_band)
                for r in range(RADIX):
                    out_ref[block, pl.ds(r, per_band, stride=RADIX), :] = rim_sum[r, rows, :] * scale
                low, high = out_ref[block, :half, :], out_ref[block, half:band_rows, :]
                out_ref[block, band_rows:, :] = low + pltpu.roll(high, LANES // 2, 1)
                for r in range(RADIX):
                    out_ref[block, pl.ds(r, per_band, stride=RADIX), :] = own_sum[r, rows, :] * scale
        else:
            for r in range(RADIX):
                outs[0][pl.ds(r, bins, stride=RADIX), :] = own_sum[r] * scale
                outs[1][pl.ds(r, bins, stride=RADIX), :] = rim_sum[r] * scale


def aligned_power(profiles, range_walk, band_order, total_batches, joined):
    batch_count, _, delays, pulses = profiles.shape
    band_count = band_order.shape[0]
    band_rows = pulses // band_count
    per_band = band_rows // RADIX
    bins, short = pulses // RADIX, pulses // RADIX
    scale = 1.0 / (total_batches * pulses)
    if delays < LANES:
        profiles = jnp.pad(profiles, ((0, 0), (0, 0), (0, LANES - delays), (0, 0)))
    if joined:
        walks = jnp.broadcast_to(range_walk[:, None], (pulses, LANES))
    else:
        picked = band_order[:, None, None] == jnp.arange(band_count, dtype=jnp.int32)[None, :, None]
        walks = jnp.sum(jnp.where(picked, range_walk.reshape(1, band_count, band_rows), 0), axis=1)
        walks = jnp.broadcast_to(walks.reshape(bins, RADIX).T[:, :, None], (RADIX, bins, LANES))
    each = 2 if batch_count % 2 == 0 else 1
    inner = np.arange(max(per_band, TILE)) % per_band
    base = (RADIX * inner[None, :] + np.arange(RADIX)[:, None]).reshape(-1)
    band = np.arange(band_count) * band_rows
    turns = np.stack(rotation(np.concatenate([base, band]), short, pulses))
    whole = lambda shape: pl.BlockSpec(shape, lambda g, order: (0,) * len(shape))
    if joined:
        shapes = ((band_count, band_rows + band_rows // 2, LANES),)
    else:
        shapes = ((pulses, LANES),) * 2
    return pl.pallas_call(
        functools.partial(power_kernel, batch_count, total_batches, per_band, scale, joined),
        out_shape=[jax.ShapeDtypeStruct(shape, jnp.float32) for shape in shapes],
        grid_spec=pltpu.PrefetchScalarGridSpec(
            num_scalar_prefetch=1,
            grid=(batch_count // each,),
            in_specs=[
                pl.BlockSpec((each, 2, LANES, pulses), lambda g, order: (g, 0, 0, 0)),
                whole(walks.shape),
                whole(turns.shape),
            ],
            out_specs=[whole(shape) for shape in shapes],
            scratch_shapes=[
                pltpu.VMEM((RADIX, bins, 2 * short), jnp.bfloat16),
                pltpu.VMEM((RADIX, 2 * LANES * each, 2 * short), jnp.bfloat16),
                pltpu.VMEM((RADIX, bins, LANES), jnp.float32),
                pltpu.VMEM((RADIX, bins, LANES), jnp.float32),
                pltpu.VMEM((RADIX, bins, LANES), jnp.int32),
            ],
        ),
        compiler_params=pltpu.CompilerParams(
            dimension_semantics=("arbitrary",), vmem_limit_bytes=48 << 20
        ),
    )(band_order, profiles, walks, jnp.asarray(turns))


MESH = pl.DeviceIdType.MESH


def bit_of(value, k):
    return lax.rem(lax.div(value, 1 << k), 2)


def flipped(value, mask):
    result = value
    for k in range(mask.bit_length()):
        if mask >> k & 1:
            result = result + (1 << k) * (1 - 2 * bit_of(value, k))
    return result


def regroup_kernel(dop_count, slow_count, data, out_ref, *refs):
    levels = slow_count.bit_length() - 1
    kept, arrived = refs[:levels], refs[levels:2 * levels]
    landed, send_sem, recv_sem = refs[2 * levels:]
    dop, slow = lax.axis_index("dop"), lax.axis_index("slow")
    band_rows = out_ref.shape[0]
    partners = [(dop, flipped(slow, 1 << k)) for k in range(levels)]
    partners += [(flipped(dop, j), slow) for j in range(1, dop_count)]

    barrier = pltpu.get_barrier_semaphore()
    for partner in partners:
        pl.semaphore_signal(barrier, inc=1, device_id=partner, device_id_type=MESH)
    pl.semaphore_wait(barrier, len(partners))

    order = list(range(dop_count - 1, -1, -1))
    copies = {}

    def send(level, j, source, target, device):
        copies[level, j] = pltpu.make_async_remote_copy(
            src_ref=source, dst_ref=target,
            send_sem=send_sem.at[level, j], recv_sem=recv_sem.at[level, j],
            device_id=device, device_id_type=MESH,
        )
        copies[level, j].start()

    for j in order:
        send(0, j, data.at[flipped(dop, j), :, 1 - bit_of(slow, 0)], arrived[0].at[j], partners[0])
    for level in range(levels):
        for j in order:
            copies[level, j].wait_recv()
            bit = bit_of(slow, level)
            held = data[flipped(dop, j), :, bit] if level == 0 else kept[level - 1][j, :, bit]
            total = held + arrived[level][j]
            if level < levels - 1:
                kept[level][j] = total.reshape(kept[level].shape[1:])
                send(
                    level + 1, j, kept[level].at[j, :, 1 - bit_of(slow, level + 1)],
                    arrived[level + 1].at[j], partners[level + 1],
                )
            elif j:
                kept[level][j] = total[0]
                send(levels, j, kept[level].at[j], landed.at[j], (flipped(dop, j), slow))
            else:
                landed[0] = total[0]
    for j in order[:-1]:
        copies[levels, j].wait_recv()

    half = band_rows // 2
    lane = lax.broadcasted_iota(jnp.int32, (half, LANES), 1)
    for e in range(dop_count):
        main = landed[flipped(dop, e), :band_rows, :]
        low = jnp.zeros((half, LANES), jnp.float32)
        high = low
        for source, mine in ((e - 1, lane < WALK), (e + 1, lane >= LANES - WALK)):
            if 0 <= source < dop_count:
                rim = landed[flipped(dop, source), band_rows:, :]
                low += jnp.where(mine, rim, 0.0)
                high += jnp.where(mine, pltpu.roll(rim, LANES // 2, 1), 0.0)
        out_ref[:half, e * LANES:(e + 1) * LANES] = main[:half] + low
        out_ref[half:, e * LANES:(e + 1) * LANES] = main[half:] + high
    for copy in copies.values():
        copy.wait_send()


def regroup(blocks, dop_count, slow_count):
    rows = blocks.shape[1]
    band_rows = rows // 3 * 2
    levels = slow_count.bit_length() - 1
    kept, arrived = [], []
    count = slow_count
    for level in range(levels):
        count //= 2
        pair = (count // 2, 2) if count > 1 else ()
        kept.append(pltpu.VMEM((dop_count, *pair, rows, LANES), jnp.float32))
        arrived.append(pltpu.VMEM((dop_count, count, rows, LANES), jnp.float32))
    return pl.pallas_call(
        functools.partial(regroup_kernel, dop_count, slow_count),
        out_shape=jax.ShapeDtypeStruct((band_rows, dop_count * LANES), jnp.float32),
        in_specs=[pl.BlockSpec(memory_space=pltpu.VMEM)],
        out_specs=pl.BlockSpec(memory_space=pltpu.VMEM),
        scratch_shapes=[
            *kept, *arrived,
            pltpu.VMEM((dop_count, rows, LANES), jnp.float32),
            pltpu.SemaphoreType.DMA((levels + 1, dop_count)),
            pltpu.SemaphoreType.DMA((levels + 1, dop_count)),
        ],
        compiler_params=pltpu.CompilerParams(
            collective_id=0, has_side_effects=True, vmem_limit_bytes=32 << 20
        ),
    )(blocks.reshape(dop_count, slow_count // 2, 2, rows, LANES))


def power_of_two(count):
    return count & (count - 1) == 0


def neighbours(value, steps):
    count = lax.axis_size("dop")
    pairs = [(source, source + steps) for source in range(count) if 0 <= source + steps < count]
    return lax.ppermute(value, "dop", pairs)


def exchange(own, rim, delays):
    dop_count, slow_count = lax.axis_size("dop"), lax.axis_size("slow")
    rows = own.shape[0] // (dop_count * slow_count)
    after = rim[:, :WALK] if delays == LANES else own[:, delays:delays + WALK]
    from_below = neighbours(after, 1)
    from_above = neighbours(rim[:, LANES - WALK:], -1)
    own = own[:, :delays].at[:, :WALK].add(from_below)
    own = own.at[:, delays - WALK:].add(from_above)
    grouped = own.reshape(dop_count, slow_count, rows, delays)
    summed = lax.psum_scatter(grouped, "slow", scatter_dimension=1, tiled=False)
    gathered = lax.all_to_all(summed, "dop", split_axis=0, concat_axis=0, tiled=True)
    return gathered.transpose(1, 0, 2).reshape(rows, dop_count * delays)


FAN = 8
NEAR_LAG = 1
HOME_LAG = 5
SUB = 8
PIECE = 32
ROWS = 16
PAIR = 2


def fan_table(pulses):
    short = pulses // FAN
    rows = (FAN * np.arange(short)[None, :] + np.arange(FAN)[:, None])[..., None]
    phases = (rows * np.arange(short)) % pulses
    angles = phases.astype(np.float32) * np.float32(2.0 * math.pi / pulses)
    return jnp.asarray(np.concatenate([np.cos(angles), np.sin(angles)], axis=2), jnp.bfloat16)


def picked(value, index):
    dims = lax.GatherDimensionNumbers(
        offset_dims=(), collapsed_slice_dims=(1,), start_index_map=(1,),
        operand_batching_dims=(0,), start_indices_batching_dims=(0,),
    )
    return lax.gather(
        value, index[..., None], dims, slice_sizes=(1, 1), mode=lax.GatherScatterMode.PROMISE_IN_BOUNDS
    )


def turned(re, im):
    half = math.sqrt(0.5)
    are = [re[q] + re[q + 4] for q in range(4)]
    aim = [im[q] + im[q + 4] for q in range(4)]
    bre = [re[q] - re[q + 4] for q in range(4)]
    bim = [im[q] - im[q + 4] for q in range(4)]
    out = [None] * FAN
    c0, c1, c2, c3 = are[0] + are[2], are[0] - are[2], are[1] + are[3], are[1] - are[3]
    s0, s1, s2, s3 = aim[0] + aim[2], aim[0] - aim[2], aim[1] + aim[3], aim[1] - aim[3]
    out[0], out[4] = (c0 + c2, s0 + s2), (c0 - c2, s0 - s2)
    out[2], out[6] = (c1 + s3, s1 - c3), (c1 - s3, s1 + c3)
    d0re, d0im, d1re, d1im = bre[0] + bim[2], bim[0] - bre[2], bre[0] - bim[2], bim[0] + bre[2]
    p1, m1 = bre[1] + bim[1], bim[1] - bre[1]
    p3, m3 = bre[3] + bim[3], bim[3] - bre[3]
    e2re, e2im = (p1 + m3) * half, (m1 - p3) * half
    e3re, e3im = (p1 - m3) * half, (m1 + p3) * half
    out[1], out[5] = (d0re + e2re, d0im + e2im), (d0re - e2re, d0im - e2im)
    out[3], out[7] = (d1re + e3im, d1im - e3re), (d1re - e3im, d1im + e3re)
    return out


def fused_body(
    accs, dop_count, total_batches, scale,
    x_hbm, table_hbm, walk_hbm, order_hbm, out_ref,
    walk_ref, order_ref, x_buf, table, y_buf, spun, walks, bases, powers, own, rim, stage,
    edges, held, near, passed, across, last, landed,
    small_sem, x_sem, table_sem, near_send, near_recv, across_send, across_recv, land_send, land_recv,
):
    batches, _, delays, pulses = x_buf.shape
    short = pulses // FAN
    pairs = batches // PAIR
    bands = order_hbm.shape[0]
    dop, slow = lax.axis_index("dop"), lax.axis_index("slow")
    core, side = lax.rem(slow, 2), lax.div(slow, 2)
    core_peer, side_peer = (dop, flipped(slow, 1)), (dop, flipped(slow, 2))
    partners = [core_peer, side_peer] + [(flipped(dop, j), slow) for j in range(1, dop_count)]
    groups = LANES // WALK

    barrier = pltpu.get_barrier_semaphore()
    for partner in partners:
        pl.semaphore_signal(barrier, inc=1, device_id=partner, device_id_type=MESH)

    small_loads = [
        pltpu.make_async_copy(walk_hbm, walk_ref, small_sem.at[0]),
        pltpu.make_async_copy(order_hbm, order_ref, small_sem.at[1]),
    ]
    table_load = pltpu.make_async_copy(table_hbm, table, table_sem)

    def load(g):
        return pltpu.make_async_copy(x_hbm.at[g], x_buf.at[g], x_sem.at[g])

    for copy in small_loads:
        copy.start()
    for g in range(batches):
        load(g).start()
    table_load.start()

    first_batch = slow * batches
    for copy in small_loads:
        copy.wait()
    for a in range(pulses // LANES):
        row = jnp.broadcast_to(walk_ref[a:a + 1, :], (LANES, LANES))
        spun[a * LANES:(a + 1) * LANES, :] = row.T

    @pl.loop(0, FAN)
    def _(r):
        walk = spun[pl.ds(r, short, stride=FAN), :]
        base = lax.broadcasted_iota(jnp.int32, walk.shape, 1) * total_batches + walk * first_batch
        walks[r] = walk.reshape(-1, SUB, LANES)
        bases[r] = base.reshape(-1, SUB, LANES)

    @pl.loop(0, batches)
    def _(g):
        load(g).wait()
        pair = lax.div(g, PAIR)
        first = lax.rem(g, PAIR) * delays

        @pl.loop(0, delays // 16)
        def _(block):
            at = pl.ds(pl.multiple_of(block * 16, 16), 16)
            to = pl.ds(pl.multiple_of(first + block * 16, 16), 16)
            for lane in range(0, short, LANES):
                parts = [
                    [
                        x_buf[g, c, at, q * short + lane:q * short + lane + LANES].astype(jnp.float32)
                        for q in range(FAN)
                    ]
                    for c in range(2)
                ]
                for r, (re, im) in enumerate(turned(*parts)):
                    y_buf[r, pair, to, lane:lane + LANES] = re.astype(jnp.bfloat16)
                    y_buf[r, pair, to, short + lane:short + lane + LANES] = im.astype(jnp.bfloat16)

    thin = lax.broadcasted_iota(jnp.int32, (SUB, LANES), 1)
    shift = total_batches.bit_length() - 1
    pieces = short // PIECE
    halves = pairs // 2

    def multiply(r, half):
        for q in range(2):
            pltpu.matmul_push_rhs(y_buf[r, 2 * half + q, :, :short], 0, q, transpose=True)
        for q in range(2):
            pltpu.matmul_push_rhs(y_buf[r, 2 * half + q, :, short:], 1, q, transpose=True)
        for register, columns in ((0, (0, 1, 1)), (1, (1, 0, -1))):
            for piece in range(pieces):
                rows = slice(piece * PIECE, (piece + 1) * PIECE)
                first = table[r, rows, columns[0] * short:(columns[0] + 1) * short]
                second = table[r, rows, columns[1] * short:(columns[1] + 1) * short]
                if columns[2] < 0:
                    second = -second
                for q in range(2):
                    re_accs, im_accs = accs[q][half % 2]
                    pltpu.matmul_acc_lhs(
                        re_accs[piece], first, load_staged_rhs=register if piece == 0 else None
                    )
                    pltpu.matmul_acc_lhs(im_accs[piece], second)

    def measure(half):
        for piece in range(pieces):
            for q in range(2):
                re, im = (pltpu.matmul_pop(sums[piece]) for sums in accs[q][half % 2])
                powers[half % 2, q, piece * PIECE:(piece + 1) * PIECE, :] = re * re + im * im

    def align(r, half):
        for piece in range(short // ROWS):
            at = slice(piece * ROWS // SUB, (piece + 1) * ROWS // SUB)
            walk = walks[r, at].reshape(ROWS, LANES)
            moved = bases[r, at].reshape(ROWS, LANES)
            if half:
                moved += walk * (2 * PAIR * half)
            own_add, rim_add = None, None
            for q in range(2):
                for b in range(PAIR):
                    if q or b:
                        moved += walk
                    power = powers[half % 2, q, piece * ROWS:(piece + 1) * ROWS, b * LANES:(b + 1) * LANES]
                    source = lax.shift_right_arithmetic(moved, shift)
                    wrapped = source & (LANES - 1)
                    value = picked(power, wrapped)
                    inside = source == wrapped
                    kept, spilled = jnp.where(inside, value, 0.0), jnp.where(inside, 0.0, value)
                    own_add = kept if own_add is None else own_add + kept
                    rim_add = spilled if rim_add is None else rim_add + spilled
            if half:
                own_add += own[at].reshape(ROWS, LANES)
                rim_add += rim[at].reshape(ROWS, LANES)
            own[at] = own_add.reshape(-1, SUB, LANES)
            rim[at] = rim_add.reshape(-1, SUB, LANES)

    def slot(band):
        owner_dop, owner_slow = divmod(band, 4)
        return owner_slow % 2, owner_dop, owner_slow // 2

    def pack(r):
        h, k = lax.div(r, groups), lax.rem(r, groups)
        mask = lax.shift_right_logical(thin, WALK.bit_length() - 1) == k
        for band in range(bands):
            source = order_ref[band]
            c, d, s = slot(band)
            held[r, c, d, s] = own[source]
            edge = rim[source]
            folded = edge + pltpu.roll(edge, WALK, 1)
            value = pltpu.roll(folded, k * WALK, 1)
            edges[c, d, s] = jnp.where(mask, value, edges[c, d, s])

        @pl.when(k == groups - 1)
        def _():
            held[FAN + h] = edges[...]

    def remote(source, target, sent, received, device):
        return pltpu.make_async_remote_copy(
            src_ref=source, dst_ref=target, send_sem=sent, recv_sem=received,
            device_id=device, device_id_type=MESH,
        )

    def near_copy(u):
        return remote(held.at[u, 1 - core], near.at[u], near_send, near_recv.at[u], core_peer)

    def across_copy(u):
        return remote(passed.at[u], across.at[u], across_send, across_recv.at[u], side_peer)

    def home_copy(u, j):
        return remote(
            last.at[u, j], landed.at[u, j], land_send, land_recv.at[u], (flipped(dop, j), slow)
        )

    def arrive(u):
        others = pl.ds(1, dop_count - 1)
        remote(last.at[u, others], landed.at[u, others], land_send, land_recv.at[u], core_peer).wait_recv()

    def send_across(u):
        near_copy(u).wait_recv()
        for d in range(dop_count):
            passed[u, d] = held[u, core, d, 1 - side] + near[u, d, 1 - side]
        across_copy(u).start()

    def send_home(u):
        across_copy(u).wait_recv()
        for j in range(dop_count - 1, -1, -1):
            d = flipped(dop, j)
            total = held[u, core, d, side] + near[u, d, side] + across[u, d]
            if j:
                last[u, j] = total
                home_copy(u, j).start()
            else:
                landed[u, 0] = total

    def both(step, r):
        step(r)
        if isinstance(r, int):
            if r % groups == groups - 1:
                step(FAN + r // groups)
        else:
            @pl.when(lax.rem(r, groups) == groups - 1)
            def _():
                step(FAN + lax.div(r, groups))

    def put(r):
        arrive(r)
        for e in range(dop_count):
            stage[e, pl.ds(r, SUB, stride=FAN), :] = landed[r, flipped(dop, e)]

    def put_rim(h):
        u = FAN + h
        arrive(u)
        mine = order_ref[dop * 4 + slow]
        for k in range(groups):
            r = h * groups + k
            walk = walks[r, mine]
            after = jnp.logical_and(walk < 0, thin < WALK)
            before = jnp.logical_and(walk > 0, thin >= LANES - WALK)
            for e in range(dop_count):
                add = 0.0
                for source, mask, move in ((e - 1, after, -k * WALK), (e + 1, before, LANES - WALK - k * WALK)):
                    if 0 <= source < dop_count:
                        value = landed[u, flipped(dop, source)]
                        if move % LANES:
                            value = pltpu.roll(value, move % LANES, 1)
                        add = add + jnp.where(mask, value, 0.0)
                at = (e, pl.ds(r, SUB, stride=FAN), slice(None))
                stage[at] = stage[at] + add

    def finish(r):
        put(r)
        if r % groups == groups - 1:
            put_rim(r // groups)

    edges[...] = jnp.zeros(edges.shape, edges.dtype)
    table_load.wait()
    multiply(0, 0)
    measure(0)
    pl.semaphore_wait(barrier, len(partners))

    @pl.loop(0, FAN)
    def _(r):
        for half in range(halves):
            if half + 1 < halves:
                multiply(r, half + 1)
            else:
                multiply(lax.rem(r + 1, FAN), 0)
            measure((half + 1) % halves)
            align(r, half)
        pack(r)
        both(lambda u: near_copy(u).start(), r)

        @pl.when(r >= NEAR_LAG)
        def _():
            both(send_across, r - NEAR_LAG)

        @pl.when(r >= HOME_LAG)
        def _():
            both(send_home, r - HOME_LAG)

    for r in range(FAN - NEAR_LAG, FAN):
        both(send_across, r)
    for r in range(FAN - HOME_LAG, FAN):
        both(send_home, r)
        if r < FAN - 1:
            finish(r - FAN + HOME_LAG)
    for r in range(HOME_LAG - 1, FAN):
        finish(r)
    for e in range(dop_count):
        out_ref[:, e * LANES:(e + 1) * LANES] = stage[e] * scale
    others = pl.ds(1, dop_count - 1)
    remote(held.at[:, 0], near, near_send, near_recv.at[0], core_peer).wait_send()
    remote(passed, across, across_send, across_recv.at[0], side_peer).wait_send()
    remote(
        last.at[:, others], landed.at[:, others], land_send, land_recv.at[0], core_peer
    ).wait_send()


def fused_kernel(dop_count, total_batches, scale, x_hbm, *refs):
    pieces = x_hbm.shape[3] // (FAN * PIECE)

    def sums(q):
        return tuple(pltpu.ACC(q)((PIECE, 2 * LANES), jnp.float32) for _ in range(pieces))

    def run(accs):
        fused_body(accs, dop_count, total_batches, scale, x_hbm, *refs)

    pl.run_scoped(run, tuple(tuple((sums(q), sums(q)) for _ in range(2)) for q in range(2)))


def fused(profiles, range_walk, band_order, dop_count, total_batches):
    batches, _, delays, pulses = profiles.shape
    bands = band_order.shape[0]
    short = pulses // FAN
    units = FAN + FAN // (LANES // WALK)
    vmem = pl.BlockSpec(memory_space=pltpu.VMEM)
    blocks = (SUB, LANES)
    f32 = jnp.float32
    return pl.pallas_call(
        functools.partial(fused_kernel, dop_count, total_batches, 1.0 / (total_batches * pulses)),
        out_shape=jax.ShapeDtypeStruct((pulses // bands, dop_count * delays), f32),
        in_specs=[pl.BlockSpec(memory_space=pltpu.HBM)] * 4,
        out_specs=vmem,
        scratch_shapes=[
            pltpu.VMEM((pulses // LANES, LANES), jnp.int32),
            pltpu.SMEM((bands,), jnp.int32),
            pltpu.VMEM(profiles.shape, jnp.bfloat16),
            pltpu.VMEM((FAN, short, 2 * short), jnp.bfloat16),
            pltpu.VMEM((FAN, batches // PAIR, PAIR * delays, 2 * short), jnp.bfloat16),
            pltpu.VMEM((pulses, LANES), jnp.int32),
            pltpu.VMEM((FAN, short // SUB, SUB, LANES), jnp.int32),
            pltpu.VMEM((FAN, short // SUB, SUB, LANES), jnp.int32),
            pltpu.VMEM((2, 2, short, PAIR * LANES), f32),
            pltpu.VMEM((short // SUB, SUB, LANES), f32),
            pltpu.VMEM((short // SUB, SUB, LANES), f32),
            pltpu.VMEM((dop_count, pulses // bands, LANES), f32),
            pltpu.VMEM((2, dop_count, 2, *blocks), f32),
            pltpu.VMEM((units, 2, dop_count, 2, *blocks), f32),
            pltpu.VMEM((units, dop_count, 2, *blocks), f32),
            pltpu.VMEM((units, dop_count, *blocks), f32),
            pltpu.VMEM((units, dop_count, *blocks), f32),
            pltpu.VMEM((units, dop_count, *blocks), f32),
            pltpu.VMEM((units, dop_count, *blocks), f32),
            pltpu.SemaphoreType.DMA((2,)),
            pltpu.SemaphoreType.DMA((batches,)),
            pltpu.SemaphoreType.DMA,
            pltpu.SemaphoreType.DMA,
            pltpu.SemaphoreType.DMA((units,)),
            pltpu.SemaphoreType.DMA,
            pltpu.SemaphoreType.DMA((units,)),
            pltpu.SemaphoreType.DMA,
            pltpu.SemaphoreType.DMA((units,)),
        ],
        compiler_params=pltpu.CompilerParams(
            collective_id=0, has_side_effects=True, vmem_limit_bytes=48 << 20
        ),
    )(*(
        pltpu.with_memory_space_constraint(value, pltpu.HBM)
        for value in (profiles, fan_table(pulses), range_walk.reshape(pulses // LANES, LANES), band_order)
    ))


def fits(profiles, band_order, dop_count, slow_count, total_batches):
    batches, _, delays, pulses = profiles.shape
    return (
        delays == LANES and pulses == 2 * LANES * FAN and batches % (2 * PAIR) == 0
        and pulses == band_order.shape[0] * SUB * FAN and band_order.shape[0] == dop_count * slow_count
        and slow_count == 4 and dop_count > 1 and power_of_two(dop_count) and power_of_two(total_batches)
    )


def on_device(profiles, range_walk, band_order):
    total_batches = profiles.shape[0] * lax.axis_size("slow")
    delays = profiles.shape[2]
    dop_count, slow_count = lax.axis_size("dop"), lax.axis_size("slow")
    if fits(profiles, band_order, dop_count, slow_count, total_batches):
        return fused(profiles, range_walk, band_order, dop_count, total_batches)
    per_band = profiles.shape[3] // (dop_count * slow_count * RADIX)
    joined = (
        delays == LANES and per_band % TILE == 0 and slow_count > 1
        and power_of_two(dop_count) and power_of_two(slow_count)
    )
    sums = aligned_power(profiles, range_walk, band_order, total_batches, joined)
    if joined:
        return regroup(sums[0], dop_count, slow_count)
    return exchange(*sums, delays)


def solution(mesh):
    placed = (P("slow", None, "dop", None), P(), P())
    return jax.shard_map(
        on_device, mesh=mesh, in_specs=placed, out_specs=P(("dop", "slow"), None), check_vma=False
    )
```

```python
import functools
import math

import jax
import jax.numpy as jnp
import numpy as np
from jax import lax
from jax.experimental import pallas as pl
from jax.experimental.pallas import tpu as pltpu
from jax.sharding import PartitionSpec as P

WALK = 32
LANES = 128
TILE = 16
RADIX = 4


def rotation(rows, pulses, length):
    phases = (np.asarray(rows)[..., None] * np.arange(pulses)) % length
    angles = phases * (2.0 * math.pi / length)
    return np.cos(angles).astype(np.float32), np.sin(angles).astype(np.float32)


def quarter_sums(x_ref, at, short):
    re = [x_ref[at, 0, :, q * short:(q + 1) * short].astype(jnp.float32) for q in range(RADIX)]
    im = [x_ref[at, 1, :, q * short:(q + 1) * short].astype(jnp.float32) for q in range(RADIX)]
    are, aim, bre, bim = re[0] + re[2], im[0] + im[2], re[0] - re[2], im[0] - im[2]
    cre, cim, dre, dim = re[1] + re[3], im[1] + im[3], re[1] - re[3], im[1] - im[3]
    return (
        (are + cre, aim + cim),
        (bre + dim, bim - dre),
        (are - cre, aim - cim),
        (bre - dim, bim + dre),
    )


def power_kernel(
    batch_count, total_batches, per_band, scale, joined,
    order_ref, x_ref, walk_ref, turns, *refs,
):
    *outs, table, packed, own_sum, rim_sum, walks = refs
    step = pl.program_id(0)
    short = x_ref.shape[3] // RADIX
    bins = table.shape[1]
    base_rows = max(per_band, TILE)
    bands_at = RADIX * base_rows

    @pl.when(step == 0)
    def _():
        own_sum[...] = jnp.zeros_like(own_sum)
        rim_sum[...] = jnp.zeros_like(rim_sum)
        row = lax.broadcasted_iota(jnp.int32, (TILE, short), 0) // min(per_band, TILE)

        @pl.loop(0, bins // TILE)
        def _(tile):
            start = pl.multiple_of(tile * TILE, TILE)
            first = start // per_band
            inside = pl.multiple_of(start % per_band, TILE) if per_band > TILE else 0
            vc = turns[0, pl.ds(bands_at + order_ref[first], 1), :]
            vs = turns[1, pl.ds(bands_at + order_ref[first], 1), :]
            for extra in range(1, max(1, TILE // per_band)):
                band = order_ref[first + extra]
                vc = jnp.where(row == extra, turns[0, pl.ds(bands_at + band, 1), :], vc)
                vs = jnp.where(row == extra, turns[1, pl.ds(bands_at + band, 1), :], vs)
            for r in range(RADIX):
                if joined:
                    at = order_ref[first] * (per_band * RADIX) + inside * RADIX + r
                    walks[r, pl.ds(start, TILE), :] = walk_ref[pl.ds(at, TILE, stride=RADIX), :]
                else:
                    walks[r, pl.ds(start, TILE), :] = walk_ref[r, pl.ds(start, TILE), :]
                bc = turns[0, pl.ds(r * base_rows + inside, TILE), :]
                bs = turns[1, pl.ds(r * base_rows + inside, TILE), :]
                table[r, pl.ds(start, TILE), :short] = (bc * vc - bs * vs).astype(jnp.bfloat16)
                table[r, pl.ds(start, TILE), short:] = (bs * vc + bc * vs).astype(jnp.bfloat16)

    each = x_ref.shape[0]
    batch = lax.axis_index("slow") * batch_count + step * each
    lane = lax.broadcasted_iota(jnp.int32, (bins, LANES), 1)
    for at in range(each):
        top, low = 2 * LANES * at, 2 * LANES * at + LANES
        for r, parts in enumerate(quarter_sums(x_ref, at, short)):
            yre, yim = (part.astype(jnp.bfloat16) for part in parts)
            packed[r, top:low, :short] = yre
            packed[r, top:low, short:] = yim
            packed[r, low:low + LANES, :short] = yim
            packed[r, low:low + LANES, short:] = -yre

    def align(r, spec):
        own_add, rim_add = 0.0, 0.0
        for at in range(each):
            re = spec[:, 2 * LANES * at:2 * LANES * at + LANES]
            im = spec[:, 2 * LANES * at + LANES:2 * LANES * (at + 1)]
            power = re * re + im * im
            moved = walks[r] * (batch + at)
            if power_of_two(total_batches):
                offset = lax.shift_right_arithmetic(moved, total_batches.bit_length() - 1)
            else:
                offset = jnp.floor_divide(moved, total_batches)
            source = lane + offset
            wrapped = source & (LANES - 1)
            value = jnp.take_along_axis(power, wrapped, axis=1, mode="promise_in_bounds")
            inside = source == wrapped
            own_add += jnp.where(inside, value, 0.0)
            rim_add += jnp.where(inside, 0.0, value)
        own_sum[r] += own_add
        rim_sum[r] += rim_add

    pending = None
    for r in range(RADIX):
        spec = lax.dot_general(
            table[r], packed[r], (((1,), (1,)), ((), ())), preferred_element_type=jnp.float32
        )
        if pending is not None:
            align(r - 1, pending)
        pending = spec
    align(RADIX - 1, pending)

    @pl.when(step == pl.num_programs(0) - 1)
    def _():
        if joined:
            out_ref = outs[0]
            band_rows = per_band * RADIX
            half = band_rows // 2

            @pl.loop(0, bins // per_band)
            def _(block):
                rows = pl.ds(pl.multiple_of(block * per_band, per_band), per_band)
                for r in range(RADIX):
                    out_ref[block, pl.ds(r, per_band, stride=RADIX), :] = rim_sum[r, rows, :] * scale
                low, high = out_ref[block, :half, :], out_ref[block, half:band_rows, :]
                out_ref[block, band_rows:, :] = low + pltpu.roll(high, LANES // 2, 1)
                for r in range(RADIX):
                    out_ref[block, pl.ds(r, per_band, stride=RADIX), :] = own_sum[r, rows, :] * scale
        else:
            for r in range(RADIX):
                outs[0][pl.ds(r, bins, stride=RADIX), :] = own_sum[r] * scale
                outs[1][pl.ds(r, bins, stride=RADIX), :] = rim_sum[r] * scale


def aligned_power(profiles, range_walk, band_order, total_batches, joined):
    batch_count, _, delays, pulses = profiles.shape
    band_count = band_order.shape[0]
    band_rows = pulses // band_count
    per_band = band_rows // RADIX
    bins, short = pulses // RADIX, pulses // RADIX
    scale = 1.0 / (total_batches * pulses)
    if delays < LANES:
        profiles = jnp.pad(profiles, ((0, 0), (0, 0), (0, LANES - delays), (0, 0)))
    if joined:
        walks = jnp.broadcast_to(range_walk[:, None], (pulses, LANES))
    else:
        picked = band_order[:, None, None] == jnp.arange(band_count, dtype=jnp.int32)[None, :, None]
        walks = jnp.sum(jnp.where(picked, range_walk.reshape(1, band_count, band_rows), 0), axis=1)
        walks = jnp.broadcast_to(walks.reshape(bins, RADIX).T[:, :, None], (RADIX, bins, LANES))
    each = 2 if batch_count % 2 == 0 else 1
    inner = np.arange(max(per_band, TILE)) % per_band
    base = (RADIX * inner[None, :] + np.arange(RADIX)[:, None]).reshape(-1)
    band = np.arange(band_count) * band_rows
    turns = np.stack(rotation(np.concatenate([base, band]), short, pulses))
    whole = lambda shape: pl.BlockSpec(shape, lambda g, order: (0,) * len(shape))
    if joined:
        shapes = ((band_count, band_rows + band_rows // 2, LANES),)
    else:
        shapes = ((pulses, LANES),) * 2
    return pl.pallas_call(
        functools.partial(power_kernel, batch_count, total_batches, per_band, scale, joined),
        out_shape=[jax.ShapeDtypeStruct(shape, jnp.float32) for shape in shapes],
        grid_spec=pltpu.PrefetchScalarGridSpec(
            num_scalar_prefetch=1,
            grid=(batch_count // each,),
            in_specs=[
                pl.BlockSpec((each, 2, LANES, pulses), lambda g, order: (g, 0, 0, 0)),
                whole(walks.shape),
                whole(turns.shape),
            ],
            out_specs=[whole(shape) for shape in shapes],
            scratch_shapes=[
                pltpu.VMEM((RADIX, bins, 2 * short), jnp.bfloat16),
                pltpu.VMEM((RADIX, 2 * LANES * each, 2 * short), jnp.bfloat16),
                pltpu.VMEM((RADIX, bins, LANES), jnp.float32),
                pltpu.VMEM((RADIX, bins, LANES), jnp.float32),
                pltpu.VMEM((RADIX, bins, LANES), jnp.int32),
            ],
        ),
        compiler_params=pltpu.CompilerParams(
            dimension_semantics=("arbitrary",), vmem_limit_bytes=48 << 20
        ),
    )(band_order, profiles, walks, jnp.asarray(turns))


MESH = pl.DeviceIdType.MESH


def bit_of(value, k):
    return lax.rem(lax.div(value, 1 << k), 2)


def flipped(value, mask):
    result = value
    for k in range(mask.bit_length()):
        if mask >> k & 1:
            result = result + (1 << k) * (1 - 2 * bit_of(value, k))
    return result


def regroup_kernel(dop_count, slow_count, data, out_ref, *refs):
    levels = slow_count.bit_length() - 1
    kept, arrived = refs[:levels], refs[levels:2 * levels]
    landed, send_sem, recv_sem = refs[2 * levels:]
    dop, slow = lax.axis_index("dop"), lax.axis_index("slow")
    band_rows = out_ref.shape[0]
    partners = [(dop, flipped(slow, 1 << k)) for k in range(levels)]
    partners += [(flipped(dop, j), slow) for j in range(1, dop_count)]

    barrier = pltpu.get_barrier_semaphore()
    for partner in partners:
        pl.semaphore_signal(barrier, inc=1, device_id=partner, device_id_type=MESH)
    pl.semaphore_wait(barrier, len(partners))

    order = list(range(dop_count - 1, -1, -1))
    copies = {}

    def send(level, j, source, target, device):
        copies[level, j] = pltpu.make_async_remote_copy(
            src_ref=source, dst_ref=target,
            send_sem=send_sem.at[level, j], recv_sem=recv_sem.at[level, j],
            device_id=device, device_id_type=MESH,
        )
        copies[level, j].start()

    for j in order:
        send(0, j, data.at[flipped(dop, j), :, 1 - bit_of(slow, 0)], arrived[0].at[j], partners[0])
    for level in range(levels):
        for j in order:
            copies[level, j].wait_recv()
            bit = bit_of(slow, level)
            held = data[flipped(dop, j), :, bit] if level == 0 else kept[level - 1][j, :, bit]
            total = held + arrived[level][j]
            if level < levels - 1:
                kept[level][j] = total.reshape(kept[level].shape[1:])
                send(
                    level + 1, j, kept[level].at[j, :, 1 - bit_of(slow, level + 1)],
                    arrived[level + 1].at[j], partners[level + 1],
                )
            elif j:
                kept[level][j] = total[0]
                send(levels, j, kept[level].at[j], landed.at[j], (flipped(dop, j), slow))
            else:
                landed[0] = total[0]
    for j in order[:-1]:
        copies[levels, j].wait_recv()

    half = band_rows // 2
    lane = lax.broadcasted_iota(jnp.int32, (half, LANES), 1)
    for e in range(dop_count):
        main = landed[flipped(dop, e), :band_rows, :]
        low = jnp.zeros((half, LANES), jnp.float32)
        high = low
        for source, mine in ((e - 1, lane < WALK), (e + 1, lane >= LANES - WALK)):
            if 0 <= source < dop_count:
                rim = landed[flipped(dop, source), band_rows:, :]
                low += jnp.where(mine, rim, 0.0)
                high += jnp.where(mine, pltpu.roll(rim, LANES // 2, 1), 0.0)
        out_ref[:half, e * LANES:(e + 1) * LANES] = main[:half] + low
        out_ref[half:, e * LANES:(e + 1) * LANES] = main[half:] + high
    for copy in copies.values():
        copy.wait_send()


def regroup(blocks, dop_count, slow_count):
    rows = blocks.shape[1]
    band_rows = rows // 3 * 2
    levels = slow_count.bit_length() - 1
    kept, arrived = [], []
    count = slow_count
    for level in range(levels):
        count //= 2
        pair = (count // 2, 2) if count > 1 else ()
        kept.append(pltpu.VMEM((dop_count, *pair, rows, LANES), jnp.float32))
        arrived.append(pltpu.VMEM((dop_count, count, rows, LANES), jnp.float32))
    return pl.pallas_call(
        functools.partial(regroup_kernel, dop_count, slow_count),
        out_shape=jax.ShapeDtypeStruct((band_rows, dop_count * LANES), jnp.float32),
        in_specs=[pl.BlockSpec(memory_space=pltpu.VMEM)],
        out_specs=pl.BlockSpec(memory_space=pltpu.VMEM),
        scratch_shapes=[
            *kept, *arrived,
            pltpu.VMEM((dop_count, rows, LANES), jnp.float32),
            pltpu.SemaphoreType.DMA((levels + 1, dop_count)),
            pltpu.SemaphoreType.DMA((levels + 1, dop_count)),
        ],
        compiler_params=pltpu.CompilerParams(
            collective_id=0, has_side_effects=True, vmem_limit_bytes=32 << 20
        ),
    )(blocks.reshape(dop_count, slow_count // 2, 2, rows, LANES))


def power_of_two(count):
    return count & (count - 1) == 0


def neighbours(value, steps):
    count = lax.axis_size("dop")
    pairs = [(source, source + steps) for source in range(count) if 0 <= source + steps < count]
    return lax.ppermute(value, "dop", pairs)


def exchange(own, rim, delays):
    dop_count, slow_count = lax.axis_size("dop"), lax.axis_size("slow")
    rows = own.shape[0] // (dop_count * slow_count)
    after = rim[:, :WALK] if delays == LANES else own[:, delays:delays + WALK]
    from_below = neighbours(after, 1)
    from_above = neighbours(rim[:, LANES - WALK:], -1)
    own = own[:, :delays].at[:, :WALK].add(from_below)
    own = own.at[:, delays - WALK:].add(from_above)
    grouped = own.reshape(dop_count, slow_count, rows, delays)
    summed = lax.psum_scatter(grouped, "slow", scatter_dimension=1, tiled=False)
    gathered = lax.all_to_all(summed, "dop", split_axis=0, concat_axis=0, tiled=True)
    return gathered.transpose(1, 0, 2).reshape(rows, dop_count * delays)


FAN = 8
NEAR_LAG = 2
HOME_LAG = 6
HOME_EARLY = 4
SUB = 8
PIECE = 32
PAIR = 2


def fan_table(pulses):
    short = pulses // FAN
    rows = (FAN * np.arange(short)[None, :] + np.arange(FAN)[:, None])[..., None]
    phases = np.swapaxes((rows * np.arange(short)) % pulses, 1, 2)
    angles = phases.astype(np.float32) * np.float32(2.0 * math.pi / pulses)
    return jnp.asarray(np.concatenate([np.cos(angles), np.sin(angles)], axis=2), jnp.bfloat16)


def picked(value, index):
    dims = lax.GatherDimensionNumbers(
        offset_dims=(), collapsed_slice_dims=(0,), start_index_map=(0,),
        operand_batching_dims=(1,), start_indices_batching_dims=(1,),
    )
    return lax.gather(
        value, index[..., None], dims, slice_sizes=(1, 1), mode=lax.GatherScatterMode.PROMISE_IN_BOUNDS
    )


def turned(re, im):
    half = math.sqrt(0.5)
    are = [re[q] + re[q + 4] for q in range(4)]
    aim = [im[q] + im[q + 4] for q in range(4)]
    bre = [re[q] - re[q + 4] for q in range(4)]
    bim = [im[q] - im[q + 4] for q in range(4)]
    out = [None] * FAN
    c0, c1, c2, c3 = are[0] + are[2], are[0] - are[2], are[1] + are[3], are[1] - are[3]
    s0, s1, s2, s3 = aim[0] + aim[2], aim[0] - aim[2], aim[1] + aim[3], aim[1] - aim[3]
    out[0], out[4] = (c0 + c2, s0 + s2), (c0 - c2, s0 - s2)
    out[2], out[6] = (c1 + s3, s1 - c3), (c1 - s3, s1 + c3)
    d0re, d0im, d1re, d1im = bre[0] + bim[2], bim[0] - bre[2], bre[0] - bim[2], bim[0] + bre[2]
    p1, m1 = bre[1] + bim[1], bim[1] - bre[1]
    p3, m3 = bre[3] + bim[3], bim[3] - bre[3]
    e2re, e2im = (p1 + m3) * half, (m1 - p3) * half
    e3re, e3im = (p1 - m3) * half, (m1 + p3) * half
    out[1], out[5] = (d0re + e2re, d0im + e2im), (d0re - e2re, d0im - e2im)
    out[3], out[7] = (d1re + e3im, d1im - e3re), (d1re - e3im, d1im + e3re)
    return out


def fused_body(
    accs, dop_count, total_batches, scale,
    x_hbm, table_hbm, walk_hbm, order_hbm, out_ref,
    walk_ref, order_ref, x_buf, table, y_buf, spun, walks, across_walks, powers, window, own_even, own_odd, rim_rows, stage,
    edges, held, near, passed, across, last, landed,
    small_sem, x_sem, table_sem, near_send, near_recv, across_send, across_recv, land_send, land_recv,
):
    batches, _, delays, pulses = x_buf.shape
    short = pulses // FAN
    pairs = batches // PAIR
    bands = order_hbm.shape[0]
    dop, slow = lax.axis_index("dop"), lax.axis_index("slow")
    core, side = lax.rem(slow, 2), lax.div(slow, 2)
    core_peer, side_peer = (dop, flipped(slow, 1)), (dop, flipped(slow, 2))
    partners = [core_peer, side_peer] + [(flipped(dop, j), slow) for j in range(1, dop_count)]
    groups = LANES // WALK
    units = FAN + FAN // groups
    owns = (own_even, own_odd)

    barrier = pltpu.get_barrier_semaphore()
    for partner in partners:
        pl.semaphore_signal(barrier, inc=1, device_id=partner, device_id_type=MESH)

    small_loads = [
        pltpu.make_async_copy(walk_hbm, walk_ref, small_sem.at[0]),
        pltpu.make_async_copy(order_hbm, order_ref, small_sem.at[1]),
    ]
    table_load = pltpu.make_async_copy(table_hbm, table, table_sem)

    def load(g):
        return pltpu.make_async_copy(x_hbm.at[g], x_buf.at[g], x_sem.at[g])

    for copy in small_loads:
        copy.start()
    for g in range(batches):
        load(g).start()
    table_load.start()

    first_batch = slow * batches
    for copy in small_loads:
        copy.wait()
    for a in range(pulses // LANES):
        row = jnp.broadcast_to(walk_ref[a:a + 1, :], (LANES, LANES))
        spun[a * LANES:(a + 1) * LANES, :] = row.T

    @pl.loop(0, FAN)
    def _(r):
        walk = spun[pl.ds(r, short, stride=FAN), :]
        walks[r] = walk.reshape(-1, SUB, LANES)
        for c in range(short // LANES):
            across_walks[r, c] = walk[c * LANES:(c + 1) * LANES, :].T[:SUB, :]

    @pl.loop(0, batches)
    def _(g):
        load(g).wait()
        pair = lax.div(g, PAIR)
        first = lax.rem(g, PAIR) * delays

        @pl.loop(0, delays // 16)
        def _(block):
            at = pl.ds(pl.multiple_of(block * 16, 16), 16)
            to = pl.ds(pl.multiple_of(first + block * 16, 16), 16)
            for lane in range(0, short, LANES):
                parts = [
                    [
                        x_buf[g, c, at, q * short + lane:q * short + lane + LANES].astype(jnp.float32)
                        for q in range(FAN)
                    ]
                    for c in range(2)
                ]
                for r, (re, im) in enumerate(turned(*parts)):
                    y_buf[r, pair, to, lane:lane + LANES] = re.astype(jnp.bfloat16)
                    y_buf[r, pair, to, short + lane:short + lane + LANES] = im.astype(jnp.bfloat16)

    thin = lax.broadcasted_iota(jnp.int32, (SUB, LANES), 1)
    shift = total_batches.bit_length() - 1
    pieces = short // PIECE
    halves = pairs // 2

    def multiply(r, half):
        cosine, sine = table[r, :, :short], table[r, :, short:]
        for q in range(2):
            pltpu.matmul_push_rhs(cosine, 0, q)
        for q in range(2):
            pltpu.matmul_push_rhs(sine, 1, q)

        def feed(q, which, part, register):
            for piece in range(pieces):
                rows = slice(piece * PIECE, (piece + 1) * PIECE)
                value = y_buf[r, 2 * half + q, rows, part * short:(part + 1) * short]
                pltpu.matmul_acc_lhs(
                    accs[q][half % 2][which][piece], value,
                    load_staged_rhs=register if piece == 0 else None,
                )

        for q in range(2):
            feed(q, 0, 0, 0)
            feed(q, 1, 1, None)
        for q in range(2):
            pltpu.matmul_push_rhs(-sine, 0, q)
        for q in range(2):
            feed(q, 0, 1, 1)
            feed(q, 1, 0, 0)

    def measure(half):
        for piece in range(pieces):
            for q in range(2):
                re, im = (pltpu.matmul_pop(sums[piece]) for sums in accs[q][half % 2])
                powers[half % 2, q, piece * PIECE:(piece + 1) * PIECE, :] = re * re + im * im

    thin_row = lax.broadcasted_iota(jnp.int32, (SUB, LANES), 0)

    def align(r, half, own):
        blocks = delays // SUB
        zero = jnp.zeros((SUB, LANES), jnp.float32)
        for c in range(short // LANES):
            walk = across_walks[r, c]

            def offset(batch):
                return lax.shift_right_arithmetic(walk * (first_batch + batch), shift)

            base = jnp.minimum(offset(0), offset(batches - 1))
            turns = []
            for q in range(2):
                for b in range(PAIR):
                    at = thin_row + (offset((2 * half + q) * PAIR + b) - base)
                    turns.append((q, b * delays, at & (SUB - 1), at < SUB))
            before = [zero] * len(turns)
            for v in range(blocks + 1):
                total = window[c, v] if half else None
                for n, (q, first, index, low) in enumerate(turns):
                    if v < blocks:
                        rows = slice(first + v * SUB, first + (v + 1) * SUB)
                        value = picked(powers[half % 2, q, rows, c * LANES:(c + 1) * LANES], index)
                    else:
                        value = zero
                    part = jnp.where(low, before[n], value)
                    before[n] = value
                    total = part if total is None else total + part
                window[c, v] = total
            if half == halves - 1:
                moved = base + WALK
                at = thin_row + (moved & (SUB - 1))
                index, low = at & (SUB - 1), at < SUB
                steps = lax.shift_right_arithmetic(moved, 3)
                fine = [picked(window[c, v], index) for v in range(blocks + 1)]
                level = {}
                for m in range(-1, blocks + 1):
                    level[m] = jnp.where(low, fine[m] if m >= 0 else zero, fine[m + 1] if m < blocks else zero)
                reach = 2 * WALK // SUB - 1
                count = (delays + 2 * WALK) // SUB
                for bit in range(3):
                    far = sum(1 << other for other in range(bit + 1, 3))
                    mask = (lax.shift_right_arithmetic(steps, bit) & 1) == 1
                    fresh = {}
                    for m in range(-reach, count - reach + far):
                        here, there = level.get(m), level.get(m + (1 << bit))
                        if here is not None or there is not None:
                            fresh[m] = jnp.where(mask, zero if there is None else there, zero if here is None else here)
                    level = fresh
                edge_blocks = WALK // SUB
                out = [level.get(e - reach, zero) for e in range(count)]
                main = jnp.concatenate(out[edge_blocks:count - edge_blocks], axis=0)
                own[c * (LANES // SUB):(c + 1) * (LANES // SUB)] = main.T.reshape(-1, SUB, LANES)
                k = lax.rem(r, groups)
                for e in range(edge_blocks):
                    rows = pl.ds(pl.multiple_of(k * WALK + e * SUB, SUB), SUB)
                    rim_rows[c, rows, :] = out[e] + out[count - edge_blocks + e]

    def slot(band):
        owner_dop, owner_slow = divmod(band, 4)
        return owner_slow % 2, owner_dop, owner_slow // 2

    def pack(u, own):
        for band in range(bands):
            held[(u, *slot(band))] = own[order_ref[band]]

    def pack_rim(h):
        for c in range(short // LANES):
            edges[c * (LANES // SUB):(c + 1) * (LANES // SUB)] = rim_rows[c].T.reshape(-1, SUB, LANES)
        for band in range(bands):
            held[(FAN + h, *slot(band))] = edges[order_ref[band]]

    def remote(source, target, sent, received, device):
        return pltpu.make_async_remote_copy(
            src_ref=source, dst_ref=target, send_sem=sent, recv_sem=received,
            device_id=device, device_id_type=MESH,
        )

    def near_copy(u):
        return remote(held.at[u, 1 - core], near.at[u], near_send, near_recv.at[u], core_peer)

    def across_copy(u):
        return remote(passed.at[u], across.at[u], across_send, across_recv.at[u], side_peer)

    def home_copy(u, j):
        return remote(
            last.at[u, j], landed.at[u, j], land_send, land_recv.at[u], (flipped(dop, j), slow)
        )

    def arrive(u):
        others = pl.ds(1, dop_count - 1)
        remote(last.at[u, others], landed.at[u, others], land_send, land_recv.at[u], core_peer).wait_recv()

    def send_across(u):
        near_copy(u).wait_recv()
        for d in range(dop_count):
            passed[u, d] = held[u, core, d, 1 - side] + near[u, d, 1 - side]
        across_copy(u).start()

    def send_home(u):
        across_copy(u).wait_recv()
        for j in range(dop_count - 1, -1, -1):
            d = flipped(dop, j)
            total = held[u, core, d, side] + near[u, d, side] + across[u, d]
            if j:
                last[u, j] = total
                home_copy(u, j).start()
            else:
                landed[u, 0] = total

    def both(step, r):
        step(r)
        if isinstance(r, int):
            if r % groups == groups - 1:
                step(FAN + r // groups)
        else:
            @pl.when(lax.rem(r, groups) == groups - 1)
            def _():
                step(FAN + lax.div(r, groups))

    def put(r):
        for e in range(dop_count):
            stage[e, pl.ds(r, SUB, stride=FAN), :] = landed[r, flipped(dop, e)]

    def put_rim(h):
        mine = order_ref[dop * 4 + slow]
        values = [landed[FAN + h, flipped(dop, e)] for e in range(dop_count)]
        for k in range(groups):
            r = h * groups + k
            walk = walks[r, mine]
            after = jnp.logical_and(walk < 0, thin < WALK)
            before = jnp.logical_and(walk > 0, thin >= LANES - WALK)
            for e in range(dop_count):
                add = 0.0
                for source, mask, move in ((e - 1, after, -k * WALK), (e + 1, before, LANES - WALK - k * WALK)):
                    if 0 <= source < dop_count:
                        value = values[source]
                        if move % LANES:
                            value = pltpu.roll(value, move % LANES, 1)
                        add = add + jnp.where(mask, value, 0.0)
                at = (e, pl.ds(r, SUB, stride=FAN), slice(None))
                stage[at] = stage[at] + add

    def finish(r):
        arrive(r)
        put(r)
        if r % groups == groups - 1:
            arrive(FAN + r // groups)
            put_rim(r // groups)

    own_odd[...] = jnp.zeros(own_odd.shape, own_odd.dtype)
    table_load.wait()
    multiply(0, 0)
    measure(0)
    pl.semaphore_wait(barrier, len(partners))

    @pl.loop(0, FAN // 2)
    def _(i):
        for odd in range(2):
            r = 2 * i + odd
            for half in range(halves):
                if half + 1 < halves:
                    multiply(r, half + 1)
                else:
                    multiply(lax.rem(r + 1, FAN), 0)
                measure((half + 1) % halves)
                align(r, half, owns[odd])
            pack(lax.rem(r + units, units + 1), owns[1 - odd])

            def start_near():
                near_copy(r - 1).start()

            if odd:
                start_near()

                @pl.when(lax.rem(r, groups) == groups - 1)
                def _():
                    pack_rim(lax.div(r, groups))
                    near_copy(FAN + lax.div(r, groups)).start()
            else:
                pl.when(i > 0)(start_near)

            @pl.when(r >= NEAR_LAG)
            def _():
                both(send_across, r - NEAR_LAG)

            @pl.when(r >= HOME_LAG)
            def _():
                both(send_home, r - HOME_LAG)

    pack(FAN - 1, owns[1])
    near_copy(FAN - 1).start()
    for r in range(FAN - NEAR_LAG, FAN - 1):
        both(send_across, r)
    for r in range(FAN - HOME_LAG, HOME_EARLY):
        both(send_home, r)
    both(send_across, FAN - 1)
    for r in range(HOME_EARLY, FAN):
        both(send_home, r)
        if r < FAN - 1:
            finish(r - HOME_EARLY)
    for r in range(FAN - 1 - HOME_EARLY, FAN):
        finish(r)
    for e in range(dop_count):
        out_ref[:, e * LANES:(e + 1) * LANES] = stage[e] * scale
    others = pl.ds(1, dop_count - 1)
    remote(held.at[pl.ds(0, units), 0], near, near_send, near_recv.at[0], core_peer).wait_send()
    remote(passed, across, across_send, across_recv.at[0], side_peer).wait_send()
    remote(
        last.at[:, others], landed.at[:, others], land_send, land_recv.at[0], core_peer
    ).wait_send()


def fused_kernel(dop_count, total_batches, scale, x_hbm, *refs):
    pieces = x_hbm.shape[3] // (FAN * PIECE)

    def sums(q):
        return tuple(pltpu.ACC(q)((PIECE, 2 * LANES), jnp.float32) for _ in range(pieces))

    def run(accs):
        fused_body(accs, dop_count, total_batches, scale, x_hbm, *refs)

    pl.run_scoped(run, tuple(tuple((sums(q), sums(q)) for _ in range(2)) for q in range(2)))


def fused(profiles, range_walk, band_order, dop_count, total_batches):
    batches, _, delays, pulses = profiles.shape
    bands = band_order.shape[0]
    short = pulses // FAN
    units = FAN + FAN // (LANES // WALK)
    vmem = pl.BlockSpec(memory_space=pltpu.VMEM)
    blocks = (SUB, LANES)
    f32 = jnp.float32
    return pl.pallas_call(
        functools.partial(fused_kernel, dop_count, total_batches, 1.0 / (total_batches * pulses)),
        out_shape=jax.ShapeDtypeStruct((pulses // bands, dop_count * delays), f32),
        in_specs=[pl.BlockSpec(memory_space=pltpu.HBM)] * 4,
        out_specs=vmem,
        scratch_shapes=[
            pltpu.VMEM((pulses // LANES, LANES), jnp.int32),
            pltpu.SMEM((bands,), jnp.int32),
            pltpu.VMEM(profiles.shape, jnp.bfloat16),
            pltpu.VMEM((FAN, short, 2 * short), jnp.bfloat16),
            pltpu.VMEM((FAN, batches // PAIR, PAIR * delays, 2 * short), jnp.bfloat16),
            pltpu.VMEM((pulses, LANES), jnp.int32),
            pltpu.VMEM((FAN, short // SUB, SUB, LANES), jnp.int32),
            pltpu.VMEM((FAN, short // LANES, SUB, LANES), jnp.int32),
            pltpu.VMEM((2, 2, short, PAIR * LANES), f32),
            pltpu.VMEM((short // LANES, delays // SUB + 1, SUB, LANES), f32),
            pltpu.VMEM((short // SUB, SUB, LANES), f32),
            pltpu.VMEM((short // SUB, SUB, LANES), f32),
            pltpu.VMEM((short // LANES, LANES, LANES), f32),
            pltpu.VMEM((dop_count, pulses // bands, LANES), f32),
            pltpu.VMEM((short // SUB, SUB, LANES), f32),
            pltpu.VMEM((units + 1, 2, dop_count, 2, *blocks), f32),
            pltpu.VMEM((units, dop_count, 2, *blocks), f32),
            pltpu.VMEM((units, dop_count, *blocks), f32),
            pltpu.VMEM((units, dop_count, *blocks), f32),
            pltpu.VMEM((units, dop_count, *blocks), f32),
            pltpu.VMEM((units, dop_count, *blocks), f32),
            pltpu.SemaphoreType.DMA((2,)),
            pltpu.SemaphoreType.DMA((batches,)),
            pltpu.SemaphoreType.DMA,
            pltpu.SemaphoreType.DMA,
            pltpu.SemaphoreType.DMA((units,)),
            pltpu.SemaphoreType.DMA,
            pltpu.SemaphoreType.DMA((units,)),
            pltpu.SemaphoreType.DMA,
            pltpu.SemaphoreType.DMA((units,)),
        ],
        compiler_params=pltpu.CompilerParams(
            collective_id=0, has_side_effects=True, vmem_limit_bytes=48 << 20
        ),
    )(*(
        pltpu.with_memory_space_constraint(value, pltpu.HBM)
        for value in (profiles, fan_table(pulses), range_walk.reshape(pulses // LANES, LANES), band_order)
    ))


def fits(profiles, band_order, dop_count, slow_count, total_batches):
    batches, _, delays, pulses = profiles.shape
    return (
        delays == LANES and pulses == 2 * LANES * FAN and batches % (2 * PAIR) == 0
        and pulses == band_order.shape[0] * SUB * FAN and band_order.shape[0] == dop_count * slow_count
        and slow_count == 4 and dop_count > 1 and power_of_two(dop_count) and power_of_two(total_batches)
    )


def on_device(profiles, range_walk, band_order):
    total_batches = profiles.shape[0] * lax.axis_size("slow")
    delays = profiles.shape[2]
    dop_count, slow_count = lax.axis_size("dop"), lax.axis_size("slow")
    if fits(profiles, band_order, dop_count, slow_count, total_batches):
        return fused(profiles, range_walk, band_order, dop_count, total_batches)
    per_band = profiles.shape[3] // (dop_count * slow_count * RADIX)
    joined = (
        delays == LANES and per_band % TILE == 0 and slow_count > 1
        and power_of_two(dop_count) and power_of_two(slow_count)
    )
    sums = aligned_power(profiles, range_walk, band_order, total_batches, joined)
    if joined:
        return regroup(sums[0], dop_count, slow_count)
    return exchange(*sums, delays)


def solution(mesh):
    placed = (P("slow", None, "dop", None), P(), P())
    return jax.shard_map(
        on_device, mesh=mesh, in_specs=placed, out_specs=P(("dop", "slow"), None), check_vma=False
    )
```

```python
import functools
import math

import jax
import jax.numpy as jnp
import numpy as np
from jax import lax
from jax.experimental import pallas as pl
from jax.experimental.pallas import tpu as pltpu
from jax.sharding import PartitionSpec as P

WALK = 32
LANES = 128
TILE = 16
RADIX = 4


def rotation(rows, pulses, length):
    phases = (np.asarray(rows)[..., None] * np.arange(pulses)) % length
    angles = phases * (2.0 * math.pi / length)
    return np.cos(angles).astype(np.float32), np.sin(angles).astype(np.float32)


def quarter_sums(x_ref, at, short):
    re = [x_ref[at, 0, :, q * short:(q + 1) * short].astype(jnp.float32) for q in range(RADIX)]
    im = [x_ref[at, 1, :, q * short:(q + 1) * short].astype(jnp.float32) for q in range(RADIX)]
    are, aim, bre, bim = re[0] + re[2], im[0] + im[2], re[0] - re[2], im[0] - im[2]
    cre, cim, dre, dim = re[1] + re[3], im[1] + im[3], re[1] - re[3], im[1] - im[3]
    return (
        (are + cre, aim + cim),
        (bre + dim, bim - dre),
        (are - cre, aim - cim),
        (bre - dim, bim + dre),
    )


def power_kernel(
    batch_count, total_batches, per_band, scale, joined,
    order_ref, x_ref, walk_ref, turns, *refs,
):
    *outs, table, packed, own_sum, rim_sum, walks = refs
    step = pl.program_id(0)
    short = x_ref.shape[3] // RADIX
    bins = table.shape[1]
    base_rows = max(per_band, TILE)
    bands_at = RADIX * base_rows

    @pl.when(step == 0)
    def _():
        own_sum[...] = jnp.zeros_like(own_sum)
        rim_sum[...] = jnp.zeros_like(rim_sum)
        row = lax.broadcasted_iota(jnp.int32, (TILE, short), 0) // min(per_band, TILE)

        @pl.loop(0, bins // TILE)
        def _(tile):
            start = pl.multiple_of(tile * TILE, TILE)
            first = start // per_band
            inside = pl.multiple_of(start % per_band, TILE) if per_band > TILE else 0
            vc = turns[0, pl.ds(bands_at + order_ref[first], 1), :]
            vs = turns[1, pl.ds(bands_at + order_ref[first], 1), :]
            for extra in range(1, max(1, TILE // per_band)):
                band = order_ref[first + extra]
                vc = jnp.where(row == extra, turns[0, pl.ds(bands_at + band, 1), :], vc)
                vs = jnp.where(row == extra, turns[1, pl.ds(bands_at + band, 1), :], vs)
            for r in range(RADIX):
                if joined:
                    at = order_ref[first] * (per_band * RADIX) + inside * RADIX + r
                    walks[r, pl.ds(start, TILE), :] = walk_ref[pl.ds(at, TILE, stride=RADIX), :]
                else:
                    walks[r, pl.ds(start, TILE), :] = walk_ref[r, pl.ds(start, TILE), :]
                bc = turns[0, pl.ds(r * base_rows + inside, TILE), :]
                bs = turns[1, pl.ds(r * base_rows + inside, TILE), :]
                table[r, pl.ds(start, TILE), :short] = (bc * vc - bs * vs).astype(jnp.bfloat16)
                table[r, pl.ds(start, TILE), short:] = (bs * vc + bc * vs).astype(jnp.bfloat16)

    each = x_ref.shape[0]
    batch = lax.axis_index("slow") * batch_count + step * each
    lane = lax.broadcasted_iota(jnp.int32, (bins, LANES), 1)
    for at in range(each):
        top, low = 2 * LANES * at, 2 * LANES * at + LANES
        for r, parts in enumerate(quarter_sums(x_ref, at, short)):
            yre, yim = (part.astype(jnp.bfloat16) for part in parts)
            packed[r, top:low, :short] = yre
            packed[r, top:low, short:] = yim
            packed[r, low:low + LANES, :short] = yim
            packed[r, low:low + LANES, short:] = -yre

    def align(r, spec):
        own_add, rim_add = 0.0, 0.0
        for at in range(each):
            re = spec[:, 2 * LANES * at:2 * LANES * at + LANES]
            im = spec[:, 2 * LANES * at + LANES:2 * LANES * (at + 1)]
            power = re * re + im * im
            moved = walks[r] * (batch + at)
            if power_of_two(total_batches):
                offset = lax.shift_right_arithmetic(moved, total_batches.bit_length() - 1)
            else:
                offset = jnp.floor_divide(moved, total_batches)
            source = lane + offset
            wrapped = source & (LANES - 1)
            value = jnp.take_along_axis(power, wrapped, axis=1, mode="promise_in_bounds")
            inside = source == wrapped
            own_add += jnp.where(inside, value, 0.0)
            rim_add += jnp.where(inside, 0.0, value)
        own_sum[r] += own_add
        rim_sum[r] += rim_add

    pending = None
    for r in range(RADIX):
        spec = lax.dot_general(
            table[r], packed[r], (((1,), (1,)), ((), ())), preferred_element_type=jnp.float32
        )
        if pending is not None:
            align(r - 1, pending)
        pending = spec
    align(RADIX - 1, pending)

    @pl.when(step == pl.num_programs(0) - 1)
    def _():
        if joined:
            out_ref = outs[0]
            band_rows = per_band * RADIX
            half = band_rows // 2

            @pl.loop(0, bins // per_band)
            def _(block):
                rows = pl.ds(pl.multiple_of(block * per_band, per_band), per_band)
                for r in range(RADIX):
                    out_ref[block, pl.ds(r, per_band, stride=RADIX), :] = rim_sum[r, rows, :] * scale
                low, high = out_ref[block, :half, :], out_ref[block, half:band_rows, :]
                out_ref[block, band_rows:, :] = low + pltpu.roll(high, LANES // 2, 1)
                for r in range(RADIX):
                    out_ref[block, pl.ds(r, per_band, stride=RADIX), :] = own_sum[r, rows, :] * scale
        else:
            for r in range(RADIX):
                outs[0][pl.ds(r, bins, stride=RADIX), :] = own_sum[r] * scale
                outs[1][pl.ds(r, bins, stride=RADIX), :] = rim_sum[r] * scale


def aligned_power(profiles, range_walk, band_order, total_batches, joined):
    batch_count, _, delays, pulses = profiles.shape
    band_count = band_order.shape[0]
    band_rows = pulses // band_count
    per_band = band_rows // RADIX
    bins, short = pulses // RADIX, pulses // RADIX
    scale = 1.0 / (total_batches * pulses)
    if delays < LANES:
        profiles = jnp.pad(profiles, ((0, 0), (0, 0), (0, LANES - delays), (0, 0)))
    if joined:
        walks = jnp.broadcast_to(range_walk[:, None], (pulses, LANES))
    else:
        picked = band_order[:, None, None] == jnp.arange(band_count, dtype=jnp.int32)[None, :, None]
        walks = jnp.sum(jnp.where(picked, range_walk.reshape(1, band_count, band_rows), 0), axis=1)
        walks = jnp.broadcast_to(walks.reshape(bins, RADIX).T[:, :, None], (RADIX, bins, LANES))
    each = 2 if batch_count % 2 == 0 else 1
    inner = np.arange(max(per_band, TILE)) % per_band
    base = (RADIX * inner[None, :] + np.arange(RADIX)[:, None]).reshape(-1)
    band = np.arange(band_count) * band_rows
    turns = np.stack(rotation(np.concatenate([base, band]), short, pulses))
    whole = lambda shape: pl.BlockSpec(shape, lambda g, order: (0,) * len(shape))
    if joined:
        shapes = ((band_count, band_rows + band_rows // 2, LANES),)
    else:
        shapes = ((pulses, LANES),) * 2
    return pl.pallas_call(
        functools.partial(power_kernel, batch_count, total_batches, per_band, scale, joined),
        out_shape=[jax.ShapeDtypeStruct(shape, jnp.float32) for shape in shapes],
        grid_spec=pltpu.PrefetchScalarGridSpec(
            num_scalar_prefetch=1,
            grid=(batch_count // each,),
            in_specs=[
                pl.BlockSpec((each, 2, LANES, pulses), lambda g, order: (g, 0, 0, 0)),
                whole(walks.shape),
                whole(turns.shape),
            ],
            out_specs=[whole(shape) for shape in shapes],
            scratch_shapes=[
                pltpu.VMEM((RADIX, bins, 2 * short), jnp.bfloat16),
                pltpu.VMEM((RADIX, 2 * LANES * each, 2 * short), jnp.bfloat16),
                pltpu.VMEM((RADIX, bins, LANES), jnp.float32),
                pltpu.VMEM((RADIX, bins, LANES), jnp.float32),
                pltpu.VMEM((RADIX, bins, LANES), jnp.int32),
            ],
        ),
        compiler_params=pltpu.CompilerParams(
            dimension_semantics=("arbitrary",), vmem_limit_bytes=48 << 20
        ),
    )(band_order, profiles, walks, jnp.asarray(turns))


MESH = pl.DeviceIdType.MESH


def bit_of(value, k):
    return lax.rem(lax.div(value, 1 << k), 2)


def flipped(value, mask):
    result = value
    for k in range(mask.bit_length()):
        if mask >> k & 1:
            result = result + (1 << k) * (1 - 2 * bit_of(value, k))
    return result


def regroup_kernel(dop_count, slow_count, data, out_ref, *refs):
    levels = slow_count.bit_length() - 1
    kept, arrived = refs[:levels], refs[levels:2 * levels]
    landed, send_sem, recv_sem = refs[2 * levels:]
    dop, slow = lax.axis_index("dop"), lax.axis_index("slow")
    band_rows = out_ref.shape[0]
    partners = [(dop, flipped(slow, 1 << k)) for k in range(levels)]
    partners += [(flipped(dop, j), slow) for j in range(1, dop_count)]

    barrier = pltpu.get_barrier_semaphore()
    for partner in partners:
        pl.semaphore_signal(barrier, inc=1, device_id=partner, device_id_type=MESH)
    pl.semaphore_wait(barrier, len(partners))

    order = list(range(dop_count - 1, -1, -1))
    copies = {}

    def send(level, j, source, target, device):
        copies[level, j] = pltpu.make_async_remote_copy(
            src_ref=source, dst_ref=target,
            send_sem=send_sem.at[level, j], recv_sem=recv_sem.at[level, j],
            device_id=device, device_id_type=MESH,
        )
        copies[level, j].start()

    for j in order:
        send(0, j, data.at[flipped(dop, j), :, 1 - bit_of(slow, 0)], arrived[0].at[j], partners[0])
    for level in range(levels):
        for j in order:
            copies[level, j].wait_recv()
            bit = bit_of(slow, level)
            held = data[flipped(dop, j), :, bit] if level == 0 else kept[level - 1][j, :, bit]
            total = held + arrived[level][j]
            if level < levels - 1:
                kept[level][j] = total.reshape(kept[level].shape[1:])
                send(
                    level + 1, j, kept[level].at[j, :, 1 - bit_of(slow, level + 1)],
                    arrived[level + 1].at[j], partners[level + 1],
                )
            elif j:
                kept[level][j] = total[0]
                send(levels, j, kept[level].at[j], landed.at[j], (flipped(dop, j), slow))
            else:
                landed[0] = total[0]
    for j in order[:-1]:
        copies[levels, j].wait_recv()

    half = band_rows // 2
    lane = lax.broadcasted_iota(jnp.int32, (half, LANES), 1)
    for e in range(dop_count):
        main = landed[flipped(dop, e), :band_rows, :]
        low = jnp.zeros((half, LANES), jnp.float32)
        high = low
        for source, mine in ((e - 1, lane < WALK), (e + 1, lane >= LANES - WALK)):
            if 0 <= source < dop_count:
                rim = landed[flipped(dop, source), band_rows:, :]
                low += jnp.where(mine, rim, 0.0)
                high += jnp.where(mine, pltpu.roll(rim, LANES // 2, 1), 0.0)
        out_ref[:half, e * LANES:(e + 1) * LANES] = main[:half] + low
        out_ref[half:, e * LANES:(e + 1) * LANES] = main[half:] + high
    for copy in copies.values():
        copy.wait_send()


def regroup(blocks, dop_count, slow_count):
    rows = blocks.shape[1]
    band_rows = rows // 3 * 2
    levels = slow_count.bit_length() - 1
    kept, arrived = [], []
    count = slow_count
    for level in range(levels):
        count //= 2
        pair = (count // 2, 2) if count > 1 else ()
        kept.append(pltpu.VMEM((dop_count, *pair, rows, LANES), jnp.float32))
        arrived.append(pltpu.VMEM((dop_count, count, rows, LANES), jnp.float32))
    return pl.pallas_call(
        functools.partial(regroup_kernel, dop_count, slow_count),
        out_shape=jax.ShapeDtypeStruct((band_rows, dop_count * LANES), jnp.float32),
        in_specs=[pl.BlockSpec(memory_space=pltpu.VMEM)],
        out_specs=pl.BlockSpec(memory_space=pltpu.VMEM),
        scratch_shapes=[
            *kept, *arrived,
            pltpu.VMEM((dop_count, rows, LANES), jnp.float32),
            pltpu.SemaphoreType.DMA((levels + 1, dop_count)),
            pltpu.SemaphoreType.DMA((levels + 1, dop_count)),
        ],
        compiler_params=pltpu.CompilerParams(
            collective_id=0, has_side_effects=True, vmem_limit_bytes=32 << 20
        ),
    )(blocks.reshape(dop_count, slow_count // 2, 2, rows, LANES))


def power_of_two(count):
    return count & (count - 1) == 0


def neighbours(value, steps):
    count = lax.axis_size("dop")
    pairs = [(source, source + steps) for source in range(count) if 0 <= source + steps < count]
    return lax.ppermute(value, "dop", pairs)


def exchange(own, rim, delays):
    dop_count, slow_count = lax.axis_size("dop"), lax.axis_size("slow")
    rows = own.shape[0] // (dop_count * slow_count)
    after = rim[:, :WALK] if delays == LANES else own[:, delays:delays + WALK]
    from_below = neighbours(after, 1)
    from_above = neighbours(rim[:, LANES - WALK:], -1)
    own = own[:, :delays].at[:, :WALK].add(from_below)
    own = own.at[:, delays - WALK:].add(from_above)
    grouped = own.reshape(dop_count, slow_count, rows, delays)
    summed = lax.psum_scatter(grouped, "slow", scatter_dimension=1, tiled=False)
    gathered = lax.all_to_all(summed, "dop", split_axis=0, concat_axis=0, tiled=True)
    return gathered.transpose(1, 0, 2).reshape(rows, dop_count * delays)


FAN = 8
NEAR_LAG = 1
HOME_LAG = 5
HOME_EARLY = 3
SUB = 8
PIECE = 32
PAIR = 2


def fan_table(pulses):
    short = pulses // FAN
    rows = (FAN * np.arange(short)[None, :] + np.arange(FAN)[:, None])[..., None]
    phases = np.swapaxes((rows * np.arange(short)) % pulses, 1, 2)
    angles = phases.astype(np.float32) * np.float32(2.0 * math.pi / pulses)
    return jnp.asarray(np.concatenate([np.cos(angles), np.sin(angles)], axis=2), jnp.bfloat16)


def picked(value, index):
    dims = lax.GatherDimensionNumbers(
        offset_dims=(), collapsed_slice_dims=(0,), start_index_map=(0,),
        operand_batching_dims=(1,), start_indices_batching_dims=(1,),
    )
    return lax.gather(
        value, index[..., None], dims, slice_sizes=(1, 1), mode=lax.GatherScatterMode.PROMISE_IN_BOUNDS
    )


def turned(re, im):
    half = math.sqrt(0.5)
    are = [re[q] + re[q + 4] for q in range(4)]
    aim = [im[q] + im[q + 4] for q in range(4)]
    bre = [re[q] - re[q + 4] for q in range(4)]
    bim = [im[q] - im[q + 4] for q in range(4)]
    out = [None] * FAN
    c0, c1, c2, c3 = are[0] + are[2], are[0] - are[2], are[1] + are[3], are[1] - are[3]
    s0, s1, s2, s3 = aim[0] + aim[2], aim[0] - aim[2], aim[1] + aim[3], aim[1] - aim[3]
    out[0], out[4] = (c0 + c2, s0 + s2), (c0 - c2, s0 - s2)
    out[2], out[6] = (c1 + s3, s1 - c3), (c1 - s3, s1 + c3)
    d0re, d0im, d1re, d1im = bre[0] + bim[2], bim[0] - bre[2], bre[0] - bim[2], bim[0] + bre[2]
    p1, m1 = bre[1] + bim[1], bim[1] - bre[1]
    p3, m3 = bre[3] + bim[3], bim[3] - bre[3]
    e2re, e2im = (p1 + m3) * half, (m1 - p3) * half
    e3re, e3im = (p1 - m3) * half, (m1 + p3) * half
    out[1], out[5] = (d0re + e2re, d0im + e2im), (d0re - e2re, d0im - e2im)
    out[3], out[7] = (d1re + e3im, d1im - e3re), (d1re - e3im, d1im + e3re)
    return out


def fused_body(
    accs, dop_count, total_batches, scale,
    x_hbm, table_hbm, walk_hbm, order_hbm, out_ref,
    walk_ref, order_ref, x_buf, table, y_buf, spun, walks, across_walks, powers, window, own_even, own_odd, rim_rows, stage,
    edges, held, near, passed, across, last, landed,
    small_sem, x_sem, table_sem, near_send, near_recv, across_send, across_recv, land_send, land_recv,
):
    batches, _, delays, pulses = x_buf.shape
    short = pulses // FAN
    pairs = batches // PAIR
    bands = order_hbm.shape[0]
    dop, slow = lax.axis_index("dop"), lax.axis_index("slow")
    core, side = lax.rem(slow, 2), lax.div(slow, 2)
    core_peer, side_peer = (dop, flipped(slow, 1)), (dop, flipped(slow, 2))
    partners = [core_peer, side_peer] + [(flipped(dop, j), slow) for j in range(1, dop_count)]
    groups = LANES // WALK
    units = FAN + FAN // groups
    owns = (own_even, own_odd)

    barrier = pltpu.get_barrier_semaphore()
    for partner in partners:
        pl.semaphore_signal(barrier, inc=1, device_id=partner, device_id_type=MESH)

    small_loads = [
        pltpu.make_async_copy(walk_hbm, walk_ref, small_sem.at[0]),
        pltpu.make_async_copy(order_hbm, order_ref, small_sem.at[1]),
    ]
    table_load = pltpu.make_async_copy(table_hbm, table, table_sem)

    def load(g):
        return pltpu.make_async_copy(x_hbm.at[g], x_buf.at[g], x_sem.at[g])

    for copy in small_loads:
        copy.start()
    for g in range(batches):
        load(g).start()
    table_load.start()

    first_batch = slow * batches
    for copy in small_loads:
        copy.wait()
    for a in range(pulses // LANES):
        row = jnp.broadcast_to(walk_ref[a:a + 1, :], (LANES, LANES))
        spun[a * LANES:(a + 1) * LANES, :] = row.T

    @pl.loop(0, FAN)
    def _(r):
        walk = spun[pl.ds(r, short, stride=FAN), :]
        walks[r] = walk.reshape(-1, SUB, LANES)
        for c in range(short // LANES):
            across_walks[r, c] = walk[c * LANES:(c + 1) * LANES, :].T[:SUB, :]

    @pl.loop(0, batches)
    def _(g):
        load(g).wait()
        pair = lax.div(g, PAIR)
        first = lax.rem(g, PAIR) * delays

        @pl.loop(0, delays // 16)
        def _(block):
            at = pl.ds(pl.multiple_of(block * 16, 16), 16)
            to = pl.ds(pl.multiple_of(first + block * 16, 16), 16)
            for lane in range(0, short, LANES):
                parts = [
                    [
                        x_buf[g, c, at, q * short + lane:q * short + lane + LANES].astype(jnp.float32)
                        for q in range(FAN)
                    ]
                    for c in range(2)
                ]
                for r, (re, im) in enumerate(turned(*parts)):
                    y_buf[r, pair, to, lane:lane + LANES] = re.astype(jnp.bfloat16)
                    y_buf[r, pair, to, short + lane:short + lane + LANES] = im.astype(jnp.bfloat16)

    thin = lax.broadcasted_iota(jnp.int32, (SUB, LANES), 1)
    shift = total_batches.bit_length() - 1
    pieces = short // PIECE
    halves = pairs // 2

    def multiply(r, half):
        cosine, sine = table[r, :, :short], table[r, :, short:]
        for q in range(2):
            pltpu.matmul_push_rhs(cosine, 0, q)
        for q in range(2):
            pltpu.matmul_push_rhs(sine, 1, q)

        def feed(q, which, part, register):
            for piece in range(pieces):
                rows = slice(piece * PIECE, (piece + 1) * PIECE)
                value = y_buf[r, 2 * half + q, rows, part * short:(part + 1) * short]
                pltpu.matmul_acc_lhs(
                    accs[q][half % 2][which][piece], value,
                    load_staged_rhs=register if piece == 0 else None,
                )

        for q in range(2):
            feed(q, 0, 0, 0)
            feed(q, 1, 1, None)
        for q in range(2):
            pltpu.matmul_push_rhs(-sine, 0, q)
        for q in range(2):
            feed(q, 0, 1, 1)
            feed(q, 1, 0, 0)

    def measure(half):
        for piece in range(pieces):
            for q in range(2):
                re, im = (pltpu.matmul_pop(sums[piece]) for sums in accs[q][half % 2])
                powers[half % 2, q, piece * PIECE:(piece + 1) * PIECE, :] = re * re + im * im

    thin_row = lax.broadcasted_iota(jnp.int32, (SUB, LANES), 0)

    def align(r, half, own):
        blocks = delays // SUB
        zero = jnp.zeros((SUB, LANES), jnp.float32)
        for c in range(short // LANES):
            walk = across_walks[r, c]

            def offset(batch):
                return lax.shift_right_arithmetic(walk * (first_batch + batch), shift)

            base = jnp.minimum(offset(0), offset(batches - 1))
            turns = []
            for q in range(2):
                for b in range(PAIR):
                    at = thin_row + (offset((2 * half + q) * PAIR + b) - base)
                    turns.append((q, b * delays, at & (SUB - 1), at < SUB))
            before = [zero] * len(turns)
            for v in range(blocks + 1):
                total = window[c, v] if half else None
                for n, (q, first, index, low) in enumerate(turns):
                    if v < blocks:
                        rows = slice(first + v * SUB, first + (v + 1) * SUB)
                        value = picked(powers[half % 2, q, rows, c * LANES:(c + 1) * LANES], index)
                    else:
                        value = zero
                    part = jnp.where(low, before[n], value)
                    before[n] = value
                    total = part if total is None else total + part
                window[c, v] = total
            if half == halves - 1:
                moved = base + WALK
                at = thin_row + (moved & (SUB - 1))
                index, low = at & (SUB - 1), at < SUB
                steps = lax.shift_right_arithmetic(moved, 3)
                fine = [picked(window[c, v], index) for v in range(blocks + 1)]
                level = {}
                for m in range(-1, blocks + 1):
                    level[m] = jnp.where(low, fine[m] if m >= 0 else zero, fine[m + 1] if m < blocks else zero)
                reach = 2 * WALK // SUB - 1
                count = (delays + 2 * WALK) // SUB
                for bit in range(3):
                    far = sum(1 << other for other in range(bit + 1, 3))
                    mask = (lax.shift_right_arithmetic(steps, bit) & 1) == 1
                    fresh = {}
                    for m in range(-reach, count - reach + far):
                        here, there = level.get(m), level.get(m + (1 << bit))
                        if here is not None or there is not None:
                            fresh[m] = jnp.where(mask, zero if there is None else there, zero if here is None else here)
                    level = fresh
                edge_blocks = WALK // SUB
                out = [level.get(e - reach, zero) for e in range(count)]
                main = jnp.concatenate(out[edge_blocks:count - edge_blocks], axis=0)
                own[c * (LANES // SUB):(c + 1) * (LANES // SUB)] = main.T.reshape(-1, SUB, LANES)
                k = lax.rem(r, groups)
                for e in range(edge_blocks):
                    rows = pl.ds(pl.multiple_of(k * WALK + e * SUB, SUB), SUB)
                    rim_rows[c, rows, :] = out[e] + out[count - edge_blocks + e]

    def slot(band):
        owner_dop, owner_slow = divmod(band, 4)
        return owner_slow % 2, owner_dop, owner_slow // 2

    def pack(u, own):
        for band in range(bands):
            held[(u, *slot(band))] = own[order_ref[band]]

    def pack_rim(h):
        for c in range(short // LANES):
            edges[c * (LANES // SUB):(c + 1) * (LANES // SUB)] = rim_rows[c].T.reshape(-1, SUB, LANES)
        for band in range(bands):
            held[(FAN + h, *slot(band))] = edges[order_ref[band]]

    def remote(source, target, sent, received, device):
        return pltpu.make_async_remote_copy(
            src_ref=source, dst_ref=target, send_sem=sent, recv_sem=received,
            device_id=device, device_id_type=MESH,
        )

    def near_copy(u):
        return remote(held.at[u, 1 - core], near.at[u], near_send, near_recv.at[u], core_peer)

    def across_copy(u):
        return remote(passed.at[u], across.at[u], across_send, across_recv.at[u], side_peer)

    def home_copy(u, j):
        return remote(
            last.at[u, j], landed.at[u, j], land_send, land_recv.at[u], (flipped(dop, j), slow)
        )

    def arrive(u):
        others = pl.ds(1, dop_count - 1)
        remote(last.at[u, others], landed.at[u, others], land_send, land_recv.at[u], core_peer).wait_recv()

    def send_across(u):
        near_copy(u).wait_recv()
        for d in range(dop_count):
            passed[u, d] = held[u, core, d, 1 - side] + near[u, d, 1 - side]
        across_copy(u).start()

    def send_home(u):
        across_copy(u).wait_recv()
        for j in range(dop_count - 1, -1, -1):
            d = flipped(dop, j)
            total = held[u, core, d, side] + near[u, d, side] + across[u, d]
            if j:
                last[u, j] = total
                home_copy(u, j).start()
            else:
                landed[u, 0] = total

    def both(step, r):
        step(r)
        if isinstance(r, int):
            if r % groups == groups - 1:
                step(FAN + r // groups)
        else:
            @pl.when(lax.rem(r, groups) == groups - 1)
            def _():
                step(FAN + lax.div(r, groups))

    def put(r):
        for e in range(dop_count):
            stage[e, pl.ds(r, SUB, stride=FAN), :] = landed[r, flipped(dop, e)]

    def put_rim(h):
        mine = order_ref[dop * 4 + slow]
        values = [landed[FAN + h, flipped(dop, e)] for e in range(dop_count)]
        for k in range(groups):
            r = h * groups + k
            walk = walks[r, mine]
            after = jnp.logical_and(walk < 0, thin < WALK)
            before = jnp.logical_and(walk > 0, thin >= LANES - WALK)
            for e in range(dop_count):
                add = 0.0
                for source, mask, move in ((e - 1, after, -k * WALK), (e + 1, before, LANES - WALK - k * WALK)):
                    if 0 <= source < dop_count:
                        value = values[source]
                        if move % LANES:
                            value = pltpu.roll(value, move % LANES, 1)
                        add = add + jnp.where(mask, value, 0.0)
                at = (e, pl.ds(r, SUB, stride=FAN), slice(None))
                stage[at] = stage[at] + add

    def finish(r):
        arrive(r)
        put(r)
        if r % groups == groups - 1:
            arrive(FAN + r // groups)
            put_rim(r // groups)

    table_load.wait()
    multiply(0, 0)
    measure(0)
    pl.semaphore_wait(barrier, len(partners))

    @pl.loop(0, FAN // 2)
    def _(i):
        for odd in range(2):
            r = 2 * i + odd
            for half in range(halves):
                if half + 1 < halves:
                    multiply(r, half + 1)
                else:
                    multiply(lax.rem(r + 1, FAN), 0)
                measure((half + 1) % halves)
                align(r, half, owns[odd])
            pack(r, owns[odd])

            near_copy(r).start()
            if odd:
                @pl.when(lax.rem(r, groups) == groups - 1)
                def _():
                    pack_rim(lax.div(r, groups))
                    near_copy(FAN + lax.div(r, groups)).start()

            @pl.when(r >= NEAR_LAG)
            def _():
                both(send_across, r - NEAR_LAG)

            @pl.when(r >= HOME_LAG)
            def _():
                both(send_home, r - HOME_LAG)

    for r in range(FAN - NEAR_LAG, FAN - 1):
        both(send_across, r)
    for r in range(FAN - HOME_LAG, HOME_EARLY):
        both(send_home, r)
    both(send_across, FAN - 1)
    for r in range(HOME_EARLY, FAN):
        both(send_home, r)
    for r in range(FAN):
        finish(r)
    for e in range(dop_count):
        out_ref[:, e * LANES:(e + 1) * LANES] = stage[e] * scale
    others = pl.ds(1, dop_count - 1)
    remote(held.at[pl.ds(0, units), 0], near, near_send, near_recv.at[0], core_peer).wait_send()
    remote(passed, across, across_send, across_recv.at[0], side_peer).wait_send()
    remote(
        last.at[:, others], landed.at[:, others], land_send, land_recv.at[0], core_peer
    ).wait_send()


def fused_kernel(dop_count, total_batches, scale, x_hbm, *refs):
    pieces = x_hbm.shape[3] // (FAN * PIECE)

    def sums(q):
        return tuple(pltpu.ACC(q)((PIECE, 2 * LANES), jnp.float32) for _ in range(pieces))

    def run(accs):
        fused_body(accs, dop_count, total_batches, scale, x_hbm, *refs)

    pl.run_scoped(run, tuple(tuple((sums(q), sums(q)) for _ in range(2)) for q in range(2)))


def fused(profiles, range_walk, band_order, dop_count, total_batches):
    batches, _, delays, pulses = profiles.shape
    bands = band_order.shape[0]
    short = pulses // FAN
    units = FAN + FAN // (LANES // WALK)
    vmem = pl.BlockSpec(memory_space=pltpu.VMEM)
    blocks = (SUB, LANES)
    f32 = jnp.float32
    return pl.pallas_call(
        functools.partial(fused_kernel, dop_count, total_batches, 1.0 / (total_batches * pulses)),
        out_shape=jax.ShapeDtypeStruct((pulses // bands, dop_count * delays), f32),
        in_specs=[pl.BlockSpec(memory_space=pltpu.HBM)] * 4,
        out_specs=vmem,
        scratch_shapes=[
            pltpu.VMEM((pulses // LANES, LANES), jnp.int32),
            pltpu.SMEM((bands,), jnp.int32),
            pltpu.VMEM(profiles.shape, jnp.bfloat16),
            pltpu.VMEM((FAN, short, 2 * short), jnp.bfloat16),
            pltpu.VMEM((FAN, batches // PAIR, PAIR * delays, 2 * short), jnp.bfloat16),
            pltpu.VMEM((pulses, LANES), jnp.int32),
            pltpu.VMEM((FAN, short // SUB, SUB, LANES), jnp.int32),
            pltpu.VMEM((FAN, short // LANES, SUB, LANES), jnp.int32),
            pltpu.VMEM((2, 2, short, PAIR * LANES), f32),
            pltpu.VMEM((short // LANES, delays // SUB + 1, SUB, LANES), f32),
            pltpu.VMEM((short // SUB, SUB, LANES), f32),
            pltpu.VMEM((short // SUB, SUB, LANES), f32),
            pltpu.VMEM((short // LANES, LANES, LANES), f32),
            pltpu.VMEM((dop_count, pulses // bands, LANES), f32),
            pltpu.VMEM((short // SUB, SUB, LANES), f32),
            pltpu.VMEM((units + 1, 2, dop_count, 2, *blocks), f32),
            pltpu.VMEM((units, dop_count, 2, *blocks), f32),
            pltpu.VMEM((units, dop_count, *blocks), f32),
            pltpu.VMEM((units, dop_count, *blocks), f32),
            pltpu.VMEM((units, dop_count, *blocks), f32),
            pltpu.VMEM((units, dop_count, *blocks), f32),
            pltpu.SemaphoreType.DMA((2,)),
            pltpu.SemaphoreType.DMA((batches,)),
            pltpu.SemaphoreType.DMA,
            pltpu.SemaphoreType.DMA,
            pltpu.SemaphoreType.DMA((units,)),
            pltpu.SemaphoreType.DMA,
            pltpu.SemaphoreType.DMA((units,)),
            pltpu.SemaphoreType.DMA,
            pltpu.SemaphoreType.DMA((units,)),
        ],
        compiler_params=pltpu.CompilerParams(
            collective_id=0, has_side_effects=True, vmem_limit_bytes=48 << 20
        ),
    )(*(
        pltpu.with_memory_space_constraint(value, pltpu.HBM)
        for value in (profiles, fan_table(pulses), range_walk.reshape(pulses // LANES, LANES), band_order)
    ))


def fits(profiles, band_order, dop_count, slow_count, total_batches):
    batches, _, delays, pulses = profiles.shape
    return (
        delays == LANES and pulses == 2 * LANES * FAN and batches % (2 * PAIR) == 0
        and pulses == band_order.shape[0] * SUB * FAN and band_order.shape[0] == dop_count * slow_count
        and slow_count == 4 and dop_count > 1 and power_of_two(dop_count) and power_of_two(total_batches)
    )


def on_device(profiles, range_walk, band_order):
    total_batches = profiles.shape[0] * lax.axis_size("slow")
    delays = profiles.shape[2]
    dop_count, slow_count = lax.axis_size("dop"), lax.axis_size("slow")
    if fits(profiles, band_order, dop_count, slow_count, total_batches):
        return fused(profiles, range_walk, band_order, dop_count, total_batches)
    per_band = profiles.shape[3] // (dop_count * slow_count * RADIX)
    joined = (
        delays == LANES and per_band % TILE == 0 and slow_count > 1
        and power_of_two(dop_count) and power_of_two(slow_count)
    )
    sums = aligned_power(profiles, range_walk, band_order, total_batches, joined)
    if joined:
        return regroup(sums[0], dop_count, slow_count)
    return exchange(*sums, delays)


def solution(mesh):
    placed = (P("slow", None, "dop", None), P(), P())
    return jax.shard_map(
        on_device, mesh=mesh, in_specs=placed, out_specs=P(("dop", "slow"), None), check_vma=False
    )
```
